32 devices in a mesh: dp: 8 (over z, y), mp: 4 (over x, core).
Axes of the slice: x: 2, y: 2, z: 4, core: 2. Of those that a mesh axis runs over, the one named last changes fastest.
Arguments:
- hidden_input: bfloat16 [8192, 24], P('dp'), may hold values from -6 to 6
- output_cotangent: bfloat16 [8192, 8192], P('dp', 'mp'), may hold values from -0.023925781 to 0.023925781
- master_weights: float32 [24, 8192], P('dp', 'mp'), may hold values from -6 to 6
- first_codes: int32 [24, 8192], P('dp', 'mp'), may hold values from 0 to 15
- second_codes: int32 [24, 8192], P('dp', 'mp'), may hold values from 0 to 15
- first_rows: float32 [24], P('dp'), may hold values from 0.001 to 0.03
- first_cols: float32 [8192], P('mp'), may hold values from 0.001 to 0.03
- second_rows: float32 [24], P('dp'), may hold values from 1e-05 to 0.001
- second_cols: float32 [8192], P('mp'), may hold values from 1e-05 to 0.001
- step_count: int32 [], replicated, may hold values from 1 to 9
Outputs:
- new_master: float32 [24, 8192], P('dp', 'mp')
- update_ratio: float32 [24, 8192], P('dp', 'mp')
- gathered_params: bfloat16 [24, 8192], P(None, 'mp')
- first_scaled: float32 [24, 8192], P('dp', 'mp')
- second_scaled: float32 [24, 8192], P('dp', 'mp')
- new_first_rows: float32 [24], P('dp')
- new_first_cols: float32 [8192], P('mp')
- new_second_rows: float32 [24], P('dp')
- new_second_cols: float32 [8192], P('mp')
The draws below stay inside these ranges and needn't reach their ends.
All inputs are finite; a program needn't handle non-finite values.
Results may differ from the reference program's by a relative error of at most 0.001.
Values may be sent and summed in bfloat16 or wider, within the bound.
A program may use at most 64 MiB of HBM per device.

```python
import math
import jax
import jax.numpy as jnp
from jax import lax

D = 8192
ROWS = 24
TOKENS = 8192


def plant(values, own_key, low, high):
    longest = values.shape.index(max(values.shape))
    spots = []
    for shift in (0, 1):
        where = [jax.random.randint(jax.random.fold_in(own_key, axis), (), 0, length) for axis, length in enumerate(values.shape)]
        where[longest] = (where[longest] + shift) % values.shape[longest]
        spots.append(tuple(where))
    return values.at[spots[0]].set(low).at[spots[1]].set(high)


def spiked(values, own_key, source, target, parts, factor):
    def block_of(axis_at):
        return (jnp.arange(values.shape[axis_at]) // (values.shape[axis_at] // parts)).reshape((-1,) + (1,) * (values.ndim - 1 - axis_at))

    one_side = jax.random.permutation(own_key, parts)[block_of(target)]
    far = (block_of(target) + parts // 2) % parts
    return jnp.where((block_of(source) == one_side) | (block_of(source) == far), factor * values, values)


def block_scale(key, extent, pieces, smallest, high):
    loudness, own = 1.0, jax.random.fold_in(key, 6)
    for axis_at, parts in pieces:
        draws = jnp.exp(jax.random.uniform(jax.random.fold_in(own, axis_at), (parts,), jnp.float32, smallest / len(pieces), high / len(pieces)))
        loudness = loudness * jnp.repeat(draws, extent[axis_at] // parts).reshape([-1 if axis == axis_at else 1 for axis in range(len(extent))])
    return loudness


def bell_draw(stream_key, dims, deviation, most, split=(), kind=jnp.bfloat16):
    values = jax.random.normal(stream_key, dims, jnp.float32) * deviation
    if len(split) > 0:
        values = block_scale(stream_key, dims, split, -0.22, 0.18) * values
    return jnp.clip(values, min=-most, max=most).astype(kind)


def noise_with(own_key, extent, deviation, reach, shards, heavy, dtype=jnp.bfloat16):
    result = deviation * jax.random.normal(own_key, extent, jnp.float32)
    if shards:
        result = result * block_scale(own_key, extent, shards, -0.22, 0.18)
    return jnp.clip(spiked(result, jax.random.fold_in(own_key, 3), *heavy), -reach, reach).astype(dtype)


def setup_inputs(seed: int = 0) -> dict:
    splits = jax.random.split(jax.random.key(seed), 11)
    return {
        "hidden_input": noise_with(splits[0], (TOKENS, ROWS), 1.0, 6.0, ((0, 8),), (0, 1, 8, 2.0)),
        "output_cotangent": bell_draw(splits[1], (TOKENS, D), 0.004, 0.023925781, ((0, 8), (1, 4))),
        "master_weights": bell_draw(splits[2], (ROWS, D), 1.0, 6.0, ((0, 8), (1, 4)), jnp.float32),
        "first_codes": plant(jax.random.randint(splits[3], (ROWS, D), 0, 16), jax.random.fold_in(splits[3], 1), 0, 15).astype(jnp.int32),
        "second_codes": plant(jax.random.randint(splits[4], (ROWS, D), 0, 16), jax.random.fold_in(splits[4], 1), 0, 15).astype(jnp.int32),
        "first_rows": jnp.clip(jnp.exp(math.log(0.03) - 3.4011973 * jax.random.uniform(splits[5], (ROWS,), jnp.float32) ** block_scale(splits[5], (ROWS,), ((0, 8),), -0.2, 0.2)), 0.001, 0.03),
        "first_cols": jnp.clip(jnp.exp(math.log(0.03) - 3.4011973 * jax.random.uniform(splits[6], (D,), jnp.float32) ** block_scale(splits[6], (D,), ((0, 4),), -0.2, 0.2)), 0.001, 0.03),
        "second_rows": jnp.clip(jnp.exp(math.log(0.001) - 4.6051703 * jax.random.uniform(splits[7], (ROWS,), jnp.float32) ** block_scale(splits[7], (ROWS,), ((0, 8),), -0.2, 0.2)), 9.999999747378752e-06, 0.001),
        "second_cols": jnp.clip(jnp.exp(math.log(0.001) - 4.6051703 * jax.random.uniform(splits[8], (D,), jnp.float32) ** block_scale(splits[8], (D,), ((0, 4),), -0.2, 0.2)), 9.999999747378752e-06, 0.001),
        "step_count": jax.random.randint(splits[9], (), 1, 10).astype(jnp.int32),
    }


def reference(hidden_input, output_cotangent, master_weights, first_codes, second_codes, first_rows, first_cols, second_rows, second_cols, step_count):
    gradient = jnp.dot(hidden_input.T, output_cotangent, preferred_element_type=jnp.float32)
    entries = gradient.shape[0] * gradient.shape[1]
    gnorm = jnp.sqrt(jnp.sum(gradient * gradient))
    clipf = jnp.minimum(1.0, 0.01 * jnp.sqrt(jnp.float32(entries)) / (gnorm + 1e-06))
    clipped = clipf * gradient
    first_old = (first_codes.astype(jnp.float32) - 7.5) / 7.5 * jnp.minimum(first_rows[:, None], first_cols[None, :])
    second_level = (second_codes.astype(jnp.float32) + 1.0) / 16.0
    second_old = second_level * second_level * jnp.minimum(second_rows[:, None], second_cols[None, :])
    first_new = 0.9 * first_old + 0.1 * clipped
    second_new = 0.95 * second_old + 0.05 * clipped * clipped
    steps = step_count.astype(jnp.float32)
    first_fix = 1.0 - jnp.power(jnp.float32(0.9), steps)
    second_fix = 1.0 - jnp.power(jnp.float32(0.95), steps)
    update_ratio = first_new / first_fix / (jnp.sqrt(second_new / second_fix) + 1e-08)
    new_master = master_weights - 0.001 * (update_ratio + 0.1 * master_weights)
    first_abs = jnp.abs(first_new)
    new_first_rows = lax.optimization_barrier(jnp.max(first_abs, axis=1))
    new_first_cols = lax.optimization_barrier(jnp.max(first_abs, axis=0))
    new_second_rows = lax.optimization_barrier(jnp.max(second_new, axis=1))
    new_second_cols = lax.optimization_barrier(jnp.max(second_new, axis=0))
    first_scaled = first_new / (jnp.minimum(new_first_rows[:, None], new_first_cols[None, :]) + 1e-08)
    second_scaled = second_new / (jnp.minimum(new_second_rows[:, None], new_second_cols[None, :]) + 1e-08)
    gathered_params = new_master.astype(jnp.bfloat16)
    return (new_master, update_ratio, gathered_params, first_scaled, second_scaled, new_first_rows, new_first_cols, new_second_rows, new_second_cols)
```

```python
import functools

import jax
import jax.numpy as jnp
from jax import lax
from jax.experimental import pallas as pl
from jax.experimental.pallas import tpu as pltpu
from jax.sharding import PartitionSpec as P

MESH = pl.DeviceIdType.MESH
F32 = jnp.float32
I16 = jnp.int16
FULL = 32767.0


SUB = 8
LANES = 128


def kernel(
    ndp,
    nmp,
    loads_per_part,
    hidden_hbm,
    cot_hbm,
    master_hbm,
    code1_hbm,
    code2_hbm,
    cols1_hbm,
    cols2_hbm,
    rows1_hbm,
    rows2_hbm,
    step_hbm,
    master_out,
    ratio_out,
    params_out,
    scaled1_out,
    scaled2_out,
    rows_out,
    cols_out,
    hidden,
    cot,
    master,
    code1,
    code2,
    rows1,
    rows2,
    step_count,
    share,
    grads,
    squares,
    packs,
    metas,
    mcodes,
    mcols,
    gq,
    gscale,
    gm,
    gmscale,
    old1,
    old2,
    weights,
    all1,
    all2,
    allw,
    wide1,
    wide2,
    in_sem,
    cot_sem,
    send_sem,
    recv_sem,
):
    dp = lax.axis_index("dp")
    mp = lax.axis_index("mp")
    ndev = ndp * nmp
    flat = dp * nmp + mp
    half, side = lax.div(dp, 2), lax.rem(dp, 2)
    rows, ncols = master.shape
    parts = ncols // (SUB * LANES)
    deep = rows * SUB
    high = parts * deep
    lines = parts * SUB
    pieces = parts * loads_per_part
    width = ncols // pieces

    def loop(count, body):
        def step(i, carry):
            body(i)
            return carry

        lax.fori_loop(0, count, step, 0, unroll=count <= 32)

    loads = [
        pltpu.make_async_copy(src, dst, in_sem.at[i])
        for i, (src, dst) in enumerate(
            (
                (hidden_hbm, hidden),
                (code1_hbm, code1),
                (code2_hbm, code2),
                (master_hbm, master),
                (cols1_hbm, mcols.at[mp, pl.ds(0, lines)]),
                (cols2_hbm, mcols.at[mp, pl.ds(lines, lines)]),
                (rows1_hbm, rows1),
                (rows2_hbm, rows2),
                (step_hbm, step_count),
            )
        )
    ]
    cot_loads = [
        pltpu.make_async_copy(
            cot_hbm.at[:, pl.ds(c * width, width)], cot.at[c], cot_sem.at[c]
        )
        for c in range(pieces)
    ]

    def peer(k):
        other = lax.rem(flat + k + 1, ndev)
        return {"dp": lax.div(other, nmp), "mp": lax.rem(other, nmp)}

    def send(src, dst, which, to):
        pltpu.make_async_remote_copy(
            src_ref=src,
            dst_ref=dst,
            send_sem=send_sem.at[which],
            recv_sem=recv_sem.at[which],
            device_id=to,
            device_id_type=MESH,
        ).start()

    def dp_peer(k):
        return {"dp": lax.rem(dp + k + 1, ndp)}

    def mp_peer(k):
        return {"mp": lax.rem(mp + k + 1, nmp)}

    barrier = pltpu.get_barrier_semaphore()
    loop(
        ndev - 1,
        lambda k: pl.semaphore_signal(
            barrier, inc=1, device_id=peer(k), device_id_type=MESH
        ),
    )

    loads[0].start()
    for copy in cot_loads:
        copy.start()
    for copy in loads[1:]:
        copy.start()

    def send_share(p):
        def body(k):
            to = lax.rem(dp + k + 1, ndp)
            send(
                share.at[p, pl.ds(pl.multiple_of(to * deep, SUB), deep)],
                grads.at[k, pl.ds(p * deep, deep)],
                0,
                {"dp": to},
            )

        return body

    loads[0].wait()
    per_piece = width // LANES
    for c in range(pieces):
        cot_loads[c].wait()
        term = jnp.dot(hidden[...], cot[c], preferred_element_type=F32)
        p = c // loads_per_part
        for i in range(per_piece):
            sub = (c % loads_per_part) * per_piece + i
            share[p, pl.ds(sub, ndp * rows, stride=SUB), :] = term[
                :, i * LANES : (i + 1) * LANES
            ]
        if c == loads_per_part - 1:
            pl.semaphore_wait(barrier, ndev - 1)
        if c % loads_per_part == loads_per_part - 1:
            loop(ndp - 1, send_share(p))

    for copy in loads[1:]:
        copy.wait()

    def dense(value, ref):
        for b in range(ncols // LANES):
            at = (b // SUB) * deep + b % SUB
            ref[pl.ds(at, rows, stride=SUB), :] = value[:, b * LANES : (b + 1) * LANES]

    dense(code1[...].astype(F32), old1)
    dense(code2[...].astype(F32), old2)
    dense(master[...], weights)

    def quantize(x):
        top = jnp.maximum(jnp.max(jnp.abs(x), axis=0, keepdims=True), 1e-30)
        code = jnp.floor(x * (FULL / top) + 0.5)
        return code.astype(jnp.int32).astype(I16), top * (1.0 / FULL)

    lane = lax.broadcasted_iota(jnp.int32, (1, LANES), 1)
    scales = jnp.zeros((1, LANES), F32)
    for r in range(rows):
        scales = jnp.where(lane == r, rows1[:, r : r + 1], scales)
        scales = jnp.where(lane == rows + r, rows2[:, r : r + 1], scales)
    coded, unit = quantize(weights[...])
    pack = (old1[...] * 16.0 + old2[...]).astype(jnp.int32).astype(I16)
    packs[half, side, 0:high] = pack
    packs[half, side, high : 2 * high] = coded
    mcodes[mp] = pack
    metas[dp, 0:1] = scales
    metas[dp, 1:2] = unit

    loop(
        ndp // 2 - 1,
        lambda k: send(
            packs.at[half, side],
            packs.at[half, side],
            2,
            {"dp": lax.rem(dp + 2 * (k + 1), ndp)},
        ),
    )
    loop(ndp - 1, lambda k: send(metas.at[dp], metas.at[dp], 4, dp_peer(k)))
    loop(nmp - 1, lambda k: send(mcodes.at[mp], mcodes.at[mp], 5, mp_peer(k)))
    loop(nmp - 1, lambda k: send(mcols.at[mp], mcols.at[mp], 6, mp_peer(k)))

    def scale(row_of, cols):
        tiles = []
        for p in range(parts):
            for r in range(rows):
                tiles.append(jnp.minimum(row_of(r), cols[p * SUB : (p + 1) * SUB]))
        return jnp.concatenate(tiles, axis=0)

    def tile(x, p, r):
        at = p * deep + r * SUB
        return x[at : at + SUB]

    def first_of(code, row_of, cols):
        return 0.9 * ((code - 7.5) / 7.5 * scale(row_of, cols))

    def second_of(code, row_of, cols):
        level = (code + 1.0) / 16.0
        return 0.95 * (level * level * scale(row_of, cols))

    def split(pack):
        both = pack.astype(jnp.int32).astype(F32)
        high_code = jnp.floor(both * 0.0625)
        return high_code, both - 16.0 * high_code

    cols1 = mcols[mp, 0:lines]
    cols2 = mcols[mp, lines : 2 * lines]
    moment1 = first_of(old1[...], lambda r: rows1[:, r : r + 1], cols1)
    moment2 = second_of(old2[...], lambda r: rows2[:, r : r + 1], cols2)
    steps = step_count[...].astype(F32)
    fix1 = 1.0 - jnp.exp(steps * jnp.log(F32(0.9)))
    fix2 = 1.0 - jnp.exp(steps * jnp.log(F32(0.95)))

    def wait_all(ref, count, which):
        blocks = ref.at[pl.ds(0, count)]
        pltpu.make_async_copy(blocks, blocks, which).wait()

    def fold(fn, first, ref, count):
        if count <= 32:
            for k in range(count):
                first = fn(first, ref[k])
            return first
        return lax.fori_loop(0, count, lambda k, x: fn(x, ref[k]), first)

    mine = pl.ds(pl.multiple_of(dp * deep, SUB), deep)
    gradient = jnp.concatenate([share[p, mine, :] for p in range(parts)], axis=0)
    wait_all(grads, ndp - 1, recv_sem.at[0])
    gradient = fold(jnp.add, gradient, grads, ndp - 1)

    squares[flat] = jnp.sum(gradient * gradient, axis=0, keepdims=True)
    loop(
        ndev - 1,
        lambda k: send(
            squares.at[flat], squares.at[flat], 1, peer(ndev - 2 - k)
        ),
    )

    coded, unit = quantize(gradient)
    gq[dp] = coded
    gm[mp] = coded
    gscale[dp] = unit
    gmscale[mp] = unit
    loop(ndp - 1, lambda k: send(gq.at[dp], gq.at[dp], 7, dp_peer(k)))
    loop(ndp - 1, lambda k: send(gscale.at[dp], gscale.at[dp], 8, dp_peer(k)))
    loop(nmp - 1, lambda k: send(gm.at[mp], gm.at[mp], 9, mp_peer(k)))
    loop(nmp - 1, lambda k: send(gmscale.at[mp], gmscale.at[mp], 10, mp_peer(k)))

    column = packs.at[:, side]
    others = column.at[pl.ds(0, ndp // 2 - 1)]
    pltpu.make_async_copy(others, others, recv_sem.at[2]).wait()
    send(column, column, 3, {"dp": dp + 1 - 2 * side})

    wait_all(metas, ndp - 1, recv_sem.at[4])
    wait_all(mcodes, nmp - 1, recv_sem.at[5])
    wait_all(mcols, nmp - 1, recv_sem.at[6])

    def prepare(j):
        meta = metas[j]
        code1, code2 = split(packs[j // 2, j % 2, 0:high])
        all1[j] = first_of(code1, lambda r: meta[0:1, r : r + 1], cols1)
        all2[j] = second_of(
            code2, lambda r: meta[0:1, rows + r : rows + r + 1], cols2
        )
        known = packs[j // 2, j % 2, high : 2 * high]
        allw[j] = known.astype(jnp.int32).astype(F32) * meta[1:2]

    def prepare_wide(k):
        code1, code2 = split(mcodes[k])
        wide1[k] = first_of(code1, lambda r: rows1[:, r : r + 1], mcols[k, 0:lines])
        wide2[k] = second_of(
            code2, lambda r: rows2[:, r : r + 1], mcols[k, lines : 2 * lines]
        )

    loop(nmp, prepare_wide)
    pltpu.make_async_copy(column, column, recv_sem.at[3]).wait()
    if ndp <= 8:
        for j in range(ndp):
            prepare(j)
    else:
        lax.fori_loop(0, ndp, lambda j, c: (prepare(j), c)[1], 0)

    wait_all(squares, ndev - 1, recv_sem.at[1])
    lanes = jnp.sum(squares[...], axis=0)
    norm = jnp.sqrt(jnp.sum(lanes, axis=1, keepdims=True))
    entries = rows * ncols * ndev
    clipf = jnp.minimum(1.0, 0.01 * jnp.sqrt(F32(entries)) / (norm + 1e-6))

    clipped = clipf * gradient
    new1 = moment1 + 0.1 * clipped
    new2 = moment2 + 0.05 * (clipped * clipped)
    ratio = new1 / fix1 / (jnp.sqrt(new2 / fix2) + 1e-8)
    old_weights = weights[...]
    master_out[...] = old_weights - 0.001 * (ratio + 0.1 * old_weights)
    ratio_out[...] = ratio

    def over_rows(x):
        tops = []
        for p in range(parts):
            top = tile(x, p, 0)
            for r in range(1, rows):
                top = jnp.maximum(top, tile(x, p, r))
            tops.append(top)
        return jnp.concatenate(tops, axis=0)

    def over_cols(x):
        tops = []
        for r in range(rows):
            top = tile(x, 0, r)
            for p in range(1, parts):
                top = jnp.maximum(top, tile(x, p, r))
            tops.append(top)
        return jnp.concatenate(tops, axis=0)

    def renew(m1, m2, code, unit):
        change = code.astype(jnp.int32).astype(F32) * (unit * clipf)
        return m1 + 0.1 * change, m2 + 0.05 * (change * change)

    wait_all(gm, nmp - 1, recv_sem.at[9])
    wait_all(gmscale, nmp - 1, recv_sem.at[10])

    def widen(k, tops):
        now1, now2 = renew(wide1[k], wide2[k], gm[k], gmscale[k])
        return (
            jnp.maximum(tops[0], over_cols(jnp.abs(now1))),
            jnp.maximum(tops[1], over_cols(now2)),
        )

    flat_top = jnp.zeros((deep, LANES), F32)
    tops = lax.fori_loop(0, nmp, widen, (flat_top, flat_top), unroll=nmp <= 8)
    toprow = jnp.concatenate(
        [
            jnp.max(x[r * SUB : (r + 1) * SUB], axis=0, keepdims=True)
            for x in tops
            for r in range(rows)
        ],
        axis=0,
    )
    toprow = jnp.broadcast_to(jnp.max(toprow, axis=1, keepdims=True), toprow.shape)
    rows_out[...] = toprow

    wait_all(gq, ndp - 1, recv_sem.at[7])
    wait_all(gscale, ndp - 1, recv_sem.at[8])

    def finish(j, tops):
        now1, now2 = renew(all1[j], all2[j], gq[j], gscale[j])
        held = allw[j]
        turn = now1 / fix1 / (jnp.sqrt(now2 / fix2) + 1e-8)
        params_out[j] = (held - 0.001 * (turn + 0.1 * held)).astype(jnp.bfloat16)
        return (
            jnp.maximum(tops[0], over_rows(jnp.abs(now1))),
            jnp.maximum(tops[1], over_rows(now2)),
        )

    flat_top = jnp.zeros((lines, LANES), F32)
    top1, top2 = lax.fori_loop(0, ndp, finish, (flat_top, flat_top), unroll=ndp <= 8)
    cols_out[0] = top1
    cols_out[1] = top2
    scaled1_out[...] = new1 / (scale(lambda r: toprow[r : r + 1], top1) + 1e-8)
    scaled2_out[...] = new2 / (
        scale(lambda r: toprow[rows + r : rows + r + 1], top2) + 1e-8
    )

    wait_all(grads, ndp - 1, send_sem.at[0])
    wait_all(squares, ndev - 1, send_sem.at[1])
    pltpu.make_async_copy(others, others, send_sem.at[2]).wait()
    pltpu.make_async_copy(column, column, send_sem.at[3]).wait()
    wait_all(metas, ndp - 1, send_sem.at[4])
    wait_all(mcodes, nmp - 1, send_sem.at[5])
    wait_all(mcols, nmp - 1, send_sem.at[6])
    wait_all(gq, ndp - 1, send_sem.at[7])
    wait_all(gscale, ndp - 1, send_sem.at[8])
    wait_all(gm, nmp - 1, send_sem.at[9])
    wait_all(gmscale, nmp - 1, send_sem.at[10])


def unpack(
    master,
    ratio,
    params,
    scaled1,
    scaled2,
    toprows,
    topcols,
    master_out,
    ratio_out,
    params_out,
    scaled1_out,
    scaled2_out,
    rows1_out,
    cols1_out,
    rows2_out,
    cols2_out,
    wide,
):
    rows, ncols = master_out.shape
    ndp = params.shape[0]
    parts = ncols // (SUB * LANES)
    deep = rows * SUB

    cols1_out[...] = topcols[0]
    cols2_out[...] = topcols[1]
    for r in range(rows):
        rows1_out[r] = jnp.max(toprows[r : r + 1, :])
        rows2_out[r] = jnp.max(toprows[rows + r : rows + r + 1, :])
    for j in range(ndp):
        block = params[j].astype(F32)
        for p in range(parts):
            wide[p, j * deep : (j + 1) * deep] = block[p * deep : (p + 1) * deep]
    for b in range(ncols // LANES):
        p, sub = b // SUB, b % SUB
        cols = slice(b * LANES, (b + 1) * LANES)
        part = pl.ds(p * deep + sub, rows, stride=SUB)
        master_out[:, cols] = master[part, :]
        ratio_out[:, cols] = ratio[part, :]
        scaled1_out[:, cols] = scaled1[part, :]
        scaled2_out[:, cols] = scaled2[part, :]
        params_out[:, cols] = wide[p, pl.ds(sub, ndp * rows, stride=SUB), :].astype(
            jnp.bfloat16
        )


def shards(
    ndp,
    nmp,
    hidden_input,
    output_cotangent,
    master_weights,
    first_codes,
    second_codes,
    first_rows,
    first_cols,
    second_rows,
    second_cols,
    step_count,
):
    rows, ncols = master_weights.shape
    tokens, width = hidden_input.shape
    parts = ncols // (SUB * LANES)
    loads = 2
    height = parts * rows * SUB
    hbm = pl.BlockSpec(memory_space=pltpu.HBM)
    smem = pl.BlockSpec(memory_space=pltpu.SMEM)
    vmem = pl.BlockSpec(memory_space=pltpu.VMEM)
    whole = jax.ShapeDtypeStruct((rows, ncols), F32)
    block = (height, LANES)
    line = (parts * SUB, LANES)
    dense = pltpu.VMEM(block, F32)
    results = pl.pallas_call(
        functools.partial(kernel, ndp, nmp, loads),
        out_shape=(
            dense,
            dense,
            pltpu.VMEM((ndp, *block), jnp.bfloat16),
            dense,
            dense,
            pltpu.VMEM((2 * rows, LANES), F32),
            pltpu.VMEM((2, *line), F32),
        ),
        in_specs=[hbm] * 10,
        out_specs=[vmem] * 7,
        scratch_shapes=[
            pltpu.VMEM((width, tokens), jnp.bfloat16),
            pltpu.VMEM((parts * loads, tokens, ncols // (parts * loads)), jnp.bfloat16),
            pltpu.VMEM((rows, ncols), F32),
            pltpu.VMEM((rows, ncols), jnp.int32),
            pltpu.VMEM((rows, ncols), jnp.int32),
            pltpu.VMEM((1, rows), F32),
            pltpu.VMEM((1, rows), F32),
            pltpu.VMEM((1, 1), jnp.int32),
            pltpu.VMEM((parts, ndp * rows * SUB, LANES), F32),
            pltpu.VMEM((ndp - 1, *block), F32),
            pltpu.VMEM((ndp * nmp, 1, LANES), F32),
            pltpu.VMEM((ndp // 2, 2, 2 * height, LANES), I16),
            pltpu.VMEM((ndp, 2, LANES), F32),
            pltpu.VMEM((nmp, *block), I16),
            pltpu.VMEM((nmp, 2 * parts * SUB, LANES), F32),
            pltpu.VMEM((ndp, *block), I16),
            pltpu.VMEM((ndp, 1, LANES), F32),
            pltpu.VMEM((nmp, *block), I16),
            pltpu.VMEM((nmp, 1, LANES), F32),
            pltpu.VMEM(block, F32),
            pltpu.VMEM(block, F32),
            pltpu.VMEM(block, F32),
            pltpu.VMEM((ndp, *block), F32),
            pltpu.VMEM((ndp, *block), F32),
            pltpu.VMEM((ndp, *block), F32),
            pltpu.VMEM((nmp, *block), F32),
            pltpu.VMEM((nmp, *block), F32),
            pltpu.SemaphoreType.DMA((9,)),
            pltpu.SemaphoreType.DMA((parts * loads,)),
            pltpu.SemaphoreType.DMA((11,)),
            pltpu.SemaphoreType.DMA((11,)),
        ],
        compiler_params=pltpu.CompilerParams(
            collective_id=0, has_side_effects=True, vmem_limit_bytes=60 * 1024 * 1024
        ),
    )(
        hidden_input.T,
        output_cotangent,
        master_weights,
        first_codes,
        second_codes,
        first_cols.reshape(line),
        second_cols.reshape(line),
        first_rows.reshape(1, rows),
        second_rows.reshape(1, rows),
        step_count.reshape(1, 1),
    )
    scales = jax.ShapeDtypeStruct((rows,), F32)
    cols = jax.ShapeDtypeStruct(line, F32)
    outs = pl.pallas_call(
        unpack,
        out_shape=(
            whole,
            whole,
            jax.ShapeDtypeStruct((ndp * rows, ncols), jnp.bfloat16),
            whole,
            whole,
            scales,
            cols,
            scales,
            cols,
        ),
        in_specs=[vmem] * 7,
        out_specs=[vmem] * 5 + [smem, vmem] * 2,
        scratch_shapes=[pltpu.VMEM((parts, ndp * rows * SUB, LANES), F32)],
        compiler_params=pltpu.CompilerParams(vmem_limit_bytes=40 * 1024 * 1024),
    )(*results)
    return (*outs[:6], outs[6].reshape(ncols), outs[7], outs[8].reshape(ncols))


def solution(mesh):
    return jax.shard_map(
        functools.partial(shards, mesh.shape["dp"], mesh.shape["mp"]),
        mesh=mesh,
        in_specs=(
            P("dp", None),
            P("dp", "mp"),
            P("dp", "mp"),
            P("dp", "mp"),
            P("dp", "mp"),
            P("dp"),
            P("mp"),
            P("dp"),
            P("mp"),
            P(),
        ),
        out_specs=(
            P("dp", "mp"),
            P("dp", "mp"),
            P(None, "mp"),
            P("dp", "mp"),
            P("dp", "mp"),
            P("dp"),
            P("mp"),
            P("dp"),
            P("mp"),
        ),
        check_vma=False,
    )
```

```python
import functools

import jax
import jax.numpy as jnp
from jax import lax
from jax.experimental import pallas as pl
from jax.experimental.pallas import tpu as pltpu
from jax.sharding import PartitionSpec as P

MESH = pl.DeviceIdType.MESH
F32 = jnp.float32
I16 = jnp.int16
FULL = 32767.0


SUB = 8
LANES = 128


def kernel(
    ndp,
    nmp,
    loads_per_part,
    hidden_hbm,
    cot_hbm,
    master_hbm,
    code1_hbm,
    code2_hbm,
    cols1_hbm,
    cols2_hbm,
    rows1_hbm,
    rows2_hbm,
    step_hbm,
    master_out,
    ratio_out,
    params_out,
    scaled1_out,
    scaled2_out,
    rows_out,
    cols_out,
    hidden,
    cot,
    master,
    code1,
    code2,
    rows1,
    rows2,
    step_count,
    share,
    coded_share,
    share_unit,
    grads,
    grad_unit,
    packs,
    metas,
    mcodes,
    mcols,
    gq,
    gm,
    gunits,
    sums,
    gmine,
    gcoded,
    old1,
    old2,
    weights,
    all1,
    all2,
    allw,
    wide1,
    wide2,
    in_sem,
    cot_sem,
    pack_sem,
    send_sem,
    recv_sem,
):
    dp = lax.axis_index("dp")
    mp = lax.axis_index("mp")
    ndev = ndp * nmp
    flat = dp * nmp + mp
    half, side = lax.div(dp, 2), lax.rem(dp, 2)
    group, core = lax.div(mp, 2), lax.rem(mp, 2)
    lead = 2 * group + 1
    nown, quarter = ndp // 2, ndp // 4
    nsum = nmp // 2 * nown
    own = dp - quarter
    owner = (core == 1) & (own >= 0) & (own < nown)
    slot = group * nown + own
    source = core * ndp + dp
    rows, ncols = master.shape
    parts = ncols // (SUB * LANES)
    deep = rows * SUB
    high = parts * deep
    lines = parts * SUB
    pieces = parts * loads_per_part
    width = ncols // pieces

    def loop(count, body):
        def step(i, carry):
            body(i)
            return carry

        lax.fori_loop(0, count, step, 0, unroll=count <= 32)

    loads = [
        pltpu.make_async_copy(src, dst, in_sem.at[i])
        for i, (src, dst) in enumerate(
            (
                (hidden_hbm, hidden),
                (code1_hbm, code1),
                (code2_hbm, code2),
                (master_hbm, master),
                (cols1_hbm, mcols.at[mp, pl.ds(0, lines)]),
                (cols2_hbm, mcols.at[mp, pl.ds(lines, lines)]),
                (rows1_hbm, rows1),
                (rows2_hbm, rows2),
                (step_hbm, step_count),
            )
        )
    ]
    cot_loads = [
        pltpu.make_async_copy(
            cot_hbm.at[:, pl.ds(c * width, width)], cot.at[c], cot_sem.at[c]
        )
        for c in range(pieces)
    ]

    def send(src, dst, which, to):
        pltpu.make_async_remote_copy(
            src_ref=src,
            dst_ref=dst,
            send_sem=send_sem.at[which],
            recv_sem=recv_sem.at[which],
            device_id=to,
            device_id_type=MESH,
        ).start()

    def dp_peer(k):
        return {"dp": lax.rem(dp + k + 1, ndp)}

    def mp_peer(k):
        return {"mp": lax.rem(mp + k + 1, nmp)}

    barrier = pltpu.get_barrier_semaphore()

    def greet(to):
        pl.semaphore_signal(barrier, inc=1, device_id=to, device_id_type=MESH)

    loop(ndp - 1, lambda k: greet(dp_peer(k)))
    loop(ndp - 1, lambda k: greet({**dp_peer(k), "mp": mp + 1 - 2 * core}))
    loop(nmp - 1, lambda k: greet(mp_peer(k)))
    greeted = 2 * (ndp - 1) + nmp - 1

    loads[0].start()
    for copy in cot_loads + loads[1:]:
        copy.start()

    def partner(o):
        return o + jnp.where(o >= quarter, 2 * quarter, 0)

    def place(j):
        middle = (j >= quarter) & (j < quarter + nown)
        o = jnp.where(middle, j - quarter, jnp.where(j < quarter, j, j - nown))
        return o, jnp.where(middle, 0, 1)

    def to_owners(body):
        def step(k):
            o = lax.rem(dp + k, nown)

            @pl.when((core == 0) | (own != o))
            def _():
                body(o, {"dp": quarter + o, "mp": lead})

        loop(nown, step)

    def send_share(p):
        to_owners(
            lambda o, to: send(
                coded_share.at[p, o],
                grads.at[source, pl.ds(p * 2 * deep, 2 * deep)],
                0,
                to,
            )
        )

    def quantize(x):
        top = jnp.maximum(jnp.max(jnp.abs(x), axis=0, keepdims=True), 1e-30)
        code = jnp.floor(x * (FULL / top) + 0.5)
        return code.astype(jnp.int32).astype(I16), top * (1.0 / FULL)

    def code_share(p):
        def body(o):
            blocks = [
                share[p, pl.ds(pl.multiple_of(j * deep, SUB), deep), :]
                for j in (quarter + o, partner(o))
            ]
            coded, unit = quantize(jnp.concatenate(blocks, axis=0))
            coded_share[p, o] = coded
            share_unit[o, p : p + 1] = unit

        return body

    def prepare_packs():
        for copy in loads[1:]:
            copy.wait()

        def dense(value, ref):
            for b in range(ncols // LANES):
                at = (b // SUB) * deep + b % SUB
                ref[pl.ds(at, rows, stride=SUB), :] = value[:, b * LANES : (b + 1) * LANES]

        dense(code1[...].astype(F32), old1)
        dense(code2[...].astype(F32), old2)
        dense(master[...], weights)

        lane = lax.broadcasted_iota(jnp.int32, (1, LANES), 1)
        scales = jnp.zeros((1, LANES), F32)
        for r in range(rows):
            scales = jnp.where(lane == r, rows1[:, r : r + 1], scales)
            scales = jnp.where(lane == rows + r, rows2[:, r : r + 1], scales)
        coded, unit = quantize(weights[...])
        for i, plane in enumerate((old1, old2)):
            code = plane[...].astype(jnp.int32).astype(I16)
            packs[half, side, i * high : (i + 1) * high] = code
            mcodes[mp, i * high : (i + 1) * high] = code
        packs[half, side, 2 * high : 3 * high] = coded
        metas[dp, 0:1] = scales
        metas[dp, 1:2] = unit

    def send_packs():
        loop(
            ndp // 2 - 1,
            lambda k: pltpu.make_async_remote_copy(
                src_ref=packs.at[half, side],
                dst_ref=packs.at[half, side],
                send_sem=send_sem.at[2],
                recv_sem=pack_sem.at[half],
                device_id={"dp": lax.rem(dp + 2 * (k + 1), ndp)},
                device_id_type=MESH,
            ).start(),
        )
        send(packs.at[half, side], packs.at[half, side], 12, {"dp": dp + 1 - 2 * side})
        loop(ndp - 1, lambda k: send(metas.at[dp], metas.at[dp], 4, dp_peer(k)))
        loop(nmp - 1, lambda k: send(mcodes.at[mp], mcodes.at[mp], 5, mp_peer(k)))
        loop(nmp - 1, lambda k: send(mcols.at[mp], mcols.at[mp], 6, mp_peer(k)))

    loads[0].wait()
    per_piece = width // LANES
    for c in range(pieces):
        cot_loads[c].wait()
        term = jnp.dot(hidden[...], cot[c], preferred_element_type=F32)
        p = c // loads_per_part
        for i in range(per_piece):
            sub = (c % loads_per_part) * per_piece + i
            share[p, pl.ds(sub, ndp * rows, stride=SUB), :] = term[
                :, i * LANES : (i + 1) * LANES
            ]
        if c % loads_per_part == loads_per_part - 1:
            loop(nown, code_share(p))
        if c == loads_per_part - 1:
            pl.semaphore_wait(barrier, greeted)
        if c % loads_per_part == loads_per_part - 1:
            send_share(p)

    to_owners(lambda o, to: send(share_unit.at[o], grad_unit.at[source], 11, to))

    prepare_packs()
    send_packs()

    def scale(row_of, cols):
        tiles = []
        for p in range(parts):
            for r in range(rows):
                tiles.append(jnp.minimum(row_of(r), cols[p * SUB : (p + 1) * SUB]))
        return jnp.concatenate(tiles, axis=0)

    def tile(x, p, r):
        at = p * deep + r * SUB
        return x[at : at + SUB]

    def first_of(code, row_of, cols):
        return 0.9 * ((code - 7.5) / 7.5 * scale(row_of, cols))

    def second_of(code, row_of, cols):
        level = (code + 1.0) / 16.0
        return 0.95 * (level * level * scale(row_of, cols))

    def number(code):
        return code.astype(jnp.int32).astype(F32)

    cols1 = mcols[mp, 0:lines]
    cols2 = mcols[mp, lines : 2 * lines]
    moment1 = first_of(old1[...], lambda r: rows1[:, r : r + 1], cols1)
    moment2 = second_of(old2[...], lambda r: rows2[:, r : r + 1], cols2)
    steps = step_count[...].astype(F32)
    fix1 = 1.0 - jnp.exp(steps * jnp.log(F32(0.9)))
    fix2 = 1.0 - jnp.exp(steps * jnp.log(F32(0.95)))

    def wait_all(ref, count, which):
        blocks = ref.at[pl.ds(0, count)]
        pltpu.make_async_copy(blocks, blocks, which).wait()

    def at_peers(first, count, body):
        def step(k):
            for c in range(2):

                @pl.when((first + k != dp) | (core != c))
                def _(c=c):
                    body(c, {"dp": first + k, "mp": 2 * group + c})

        loop(count, step)

    def across(t, body):
        row = partner(own) if t else dp

        def step(to):
            for c in range(2):

                @pl.when((to != 2 * group + c) & ((t == 1) | (to != mp)))
                def _(c=c):
                    body(c, {"dp": row, "mp": to})

        loop(nmp, step)

    def gathers(near, far):
        at_peers(0, quarter, near)
        across(1, functools.partial(far, 1))
        at_peers(quarter, ndp - quarter, near)
        across(0, functools.partial(far, 0))

    def to_all(body):
        def step(k):
            @pl.when(k != flat)
            def _():
                body({"dp": lax.div(k, nmp), "mp": lax.rem(k, nmp)})

        loop(ndev, step)

    @pl.when(owner)
    def _():
        for p in range(parts):
            grads[source, p * 2 * deep : (p + 1) * 2 * deep] = coded_share[p, own]
        grad_unit[source] = share_unit[own]
        wait_all(grads, 2 * ndp - 1, recv_sem.at[0])
        wait_all(grad_unit, 2 * ndp - 1, recv_sem.at[11])
        lanes = jnp.zeros((1, LANES), F32)
        for c in range(2):

            def add(d, total, c=c):
                k = c * ndp + d
                sizes = [
                    jnp.broadcast_to(grad_unit[k, p : p + 1], (2 * deep, LANES))
                    for p in range(parts)
                ]
                return total + number(grads[k]) * jnp.concatenate(sizes, axis=0)

            total = jnp.zeros((2 * high, LANES), F32)
            total = lax.fori_loop(0, ndp, add, total, unroll=ndp <= 8)
            gmine[c] = total
            lanes = lanes + jnp.sum(total * total, axis=0, keepdims=True)
        sums[slot] = lanes
        to_all(lambda to: send(sums.at[slot], sums.at[slot], 1, to))
        for c in range(2):
            coded, unit = quantize(gmine[c])
            gunits[slot, c : c + 1] = unit
            for t in range(2):
                for p in range(parts):
                    at = (p * 2 + t) * deep
                    gcoded[c, t, p * deep : (p + 1) * deep] = coded[at : at + deep]
        to_all(lambda to: send(gunits.at[slot], gunits.at[slot], 8, to))
        gq[own] = gcoded[1]
        gm[mp - 1] = gcoded[0, 0]
        gathers(
            lambda c, to: send(gcoded.at[c], gq.at[own], 7, to),
            lambda t, c, to: send(gcoded.at[c, t], gm.at[2 * group + c], 9, to),
        )

    column = packs.at[:, side]
    others = column.at[pl.ds(0, ndp // 2 - 1)]
    pair = {"dp": dp + 1 - 2 * side}

    def relay():
        def forward(k):
            ahead = jnp.where(2 * half < ndp // 2, k + 1, ndp // 2 - k - 1)
            at = lax.rem(half + ahead, ndp // 2)
            block = packs.at[at, side]
            pltpu.make_async_copy(block, block, pack_sem.at[at]).wait()
            send(block, block, 3, pair)

        loop(ndp // 2 - 1, forward)

    relay()
    wait_all(metas, ndp - 1, recv_sem.at[4])
    wait_all(mcodes, nmp - 1, recv_sem.at[5])
    wait_all(mcols, nmp - 1, recv_sem.at[6])

    def prepare(j):
        meta = metas[j]
        code1 = number(packs[j // 2, j % 2, 0:high])
        code2 = number(packs[j // 2, j % 2, high : 2 * high])
        all1[j] = first_of(code1, lambda r: meta[0:1, r : r + 1], cols1)
        all2[j] = second_of(
            code2, lambda r: meta[0:1, rows + r : rows + r + 1], cols2
        )
        allw[j] = number(packs[j // 2, j % 2, 2 * high : 3 * high]) * meta[1:2]

    def prepare_wide(k):
        code1, code2 = number(mcodes[k, 0:high]), number(mcodes[k, high : 2 * high])
        wide1[k] = first_of(code1, lambda r: rows1[:, r : r + 1], mcols[k, 0:lines])
        wide2[k] = second_of(
            code2, lambda r: rows2[:, r : r + 1], mcols[k, lines : 2 * lines]
        )

    loop(nmp, prepare_wide)
    pltpu.make_async_copy(others, others, recv_sem.at[3]).wait()
    single = packs.at[half, side]
    pltpu.make_async_copy(single, single, recv_sem.at[12]).wait()
    if ndp <= 8:
        for j in range(ndp):
            prepare(j)
    else:
        lax.fori_loop(0, ndp, lambda j, c: (prepare(j), c)[1], 0)

    def settle(ref, count, which):
        @pl.when(owner)
        def _():
            wait_all(ref, count - 1, recv_sem.at[which])

        @pl.when(jnp.logical_not(owner))
        def _():
            wait_all(ref, count, recv_sem.at[which])

    settle(sums, nsum, 1)
    lanes = jnp.sum(sums[...], axis=0)
    norm = jnp.sqrt(jnp.sum(lanes, axis=1, keepdims=True))
    entries = rows * ncols * ndev
    clipf = jnp.minimum(1.0, 0.01 * jnp.sqrt(F32(entries)) / (norm + 1e-6))

    def over_rows(x):
        tops = []
        for p in range(parts):
            top = tile(x, p, 0)
            for r in range(1, rows):
                top = jnp.maximum(top, tile(x, p, r))
            tops.append(top)
        return jnp.concatenate(tops, axis=0)

    def over_cols(x):
        tops = []
        for r in range(rows):
            top = tile(x, 0, r)
            for p in range(1, parts):
                top = jnp.maximum(top, tile(x, p, r))
            tops.append(top)
        return jnp.concatenate(tops, axis=0)

    def renew(m1, m2, code, unit):
        change = number(code) * (unit * clipf)
        return m1 + 0.1 * change, m2 + 0.05 * (change * change)

    settle(gunits, nsum, 8)
    settle(gq, nown, 7)
    settle(gm, nmp - 1, 9)
    mine, which = place(dp)
    gm[mp] = gq[mine, which]

    gradient = number(gq[mine, which]) * gunits[group * nown + mine, pl.ds(core, 1)]
    clipped = clipf * gradient
    new1 = moment1 + 0.1 * clipped
    new2 = moment2 + 0.05 * (clipped * clipped)
    ratio = new1 / fix1 / (jnp.sqrt(new2 / fix2) + 1e-8)
    old_weights = weights[...]
    master_out[...] = old_weights - 0.001 * (ratio + 0.1 * old_weights)
    ratio_out[...] = ratio

    def widen(k, tops):
        unit = gunits[k // 2 * nown + mine, pl.ds(k % 2, 1)]
        now1, now2 = renew(wide1[k], wide2[k], gm[k], unit)
        return (
            jnp.maximum(tops[0], over_cols(jnp.abs(now1))),
            jnp.maximum(tops[1], over_cols(now2)),
        )

    flat_top = jnp.zeros((deep, LANES), F32)
    tops = lax.fori_loop(0, nmp, widen, (flat_top, flat_top), unroll=nmp <= 8)
    toprow = jnp.concatenate(
        [
            jnp.max(x[r * SUB : (r + 1) * SUB], axis=0, keepdims=True)
            for x in tops
            for r in range(rows)
        ],
        axis=0,
    )
    toprow = jnp.broadcast_to(jnp.max(toprow, axis=1, keepdims=True), toprow.shape)
    rows_out[...] = toprow

    def finish(j, tops):
        o, t = place(j)
        unit = gunits[group * nown + o, pl.ds(core, 1)]
        now1, now2 = renew(all1[j], all2[j], gq[o, t], unit)
        held = allw[j]
        turn = now1 / fix1 / (jnp.sqrt(now2 / fix2) + 1e-8)
        params_out[j] = (held - 0.001 * (turn + 0.1 * held)).astype(jnp.bfloat16)
        return (
            jnp.maximum(tops[0], over_rows(jnp.abs(now1))),
            jnp.maximum(tops[1], over_rows(now2)),
        )

    flat_top = jnp.zeros((lines, LANES), F32)
    top1, top2 = lax.fori_loop(0, ndp, finish, (flat_top, flat_top), unroll=ndp <= 8)
    cols_out[0] = top1
    cols_out[1] = top2
    scaled1_out[...] = new1 / (scale(lambda r: toprow[r : r + 1], top1) + 1e-8)
    scaled2_out[...] = new2 / (
        scale(lambda r: toprow[rows + r : rows + r + 1], top2) + 1e-8
    )

    def drain(ref, which):
        pltpu.make_async_copy(ref, ref, send_sem.at[which]).wait()

    for p in range(parts):
        to_owners(lambda o, to: drain(coded_share.at[p, o], 0))
    to_owners(lambda o, to: drain(share_unit.at[o], 11))

    @pl.when(owner)
    def _():
        loop(ndev - 1, lambda k: drain(sums.at[slot], 1))
        loop(ndev - 1, lambda k: drain(gunits.at[slot], 8))
        gathers(
            lambda c, to: drain(gcoded.at[c], 7),
            lambda t, c, to: drain(gcoded.at[c, t], 9),
        )

    pltpu.make_async_copy(others, others, send_sem.at[2]).wait()
    pltpu.make_async_copy(others, others, send_sem.at[3]).wait()
    pltpu.make_async_copy(single, single, send_sem.at[12]).wait()
    wait_all(metas, ndp - 1, send_sem.at[4])
    wait_all(mcodes, nmp - 1, send_sem.at[5])
    wait_all(mcols, nmp - 1, send_sem.at[6])


def unpack(
    master,
    ratio,
    params,
    scaled1,
    scaled2,
    toprows,
    topcols,
    master_out,
    ratio_out,
    params_out,
    scaled1_out,
    scaled2_out,
    rows1_out,
    cols1_out,
    rows2_out,
    cols2_out,
    wide,
):
    rows, ncols = master_out.shape
    ndp = params.shape[0]
    parts = ncols // (SUB * LANES)
    deep = rows * SUB

    cols1_out[...] = topcols[0]
    cols2_out[...] = topcols[1]
    for r in range(rows):
        rows1_out[r] = jnp.max(toprows[r : r + 1, :])
        rows2_out[r] = jnp.max(toprows[rows + r : rows + r + 1, :])
    for j in range(ndp):
        block = params[j].astype(F32)
        for p in range(parts):
            wide[p, j * deep : (j + 1) * deep] = block[p * deep : (p + 1) * deep]
    for b in range(ncols // LANES):
        p, sub = b // SUB, b % SUB
        cols = slice(b * LANES, (b + 1) * LANES)
        part = pl.ds(p * deep + sub, rows, stride=SUB)
        master_out[:, cols] = master[part, :]
        ratio_out[:, cols] = ratio[part, :]
        scaled1_out[:, cols] = scaled1[part, :]
        scaled2_out[:, cols] = scaled2[part, :]
        params_out[:, cols] = wide[p, pl.ds(sub, ndp * rows, stride=SUB), :].astype(
            jnp.bfloat16
        )


def shards(
    ndp,
    nmp,
    hidden_input,
    output_cotangent,
    master_weights,
    first_codes,
    second_codes,
    first_rows,
    first_cols,
    second_rows,
    second_cols,
    step_count,
):
    rows, ncols = master_weights.shape
    tokens, width = hidden_input.shape
    parts = ncols // (SUB * LANES)
    loads = 2
    height = parts * rows * SUB
    hbm = pl.BlockSpec(memory_space=pltpu.HBM)
    smem = pl.BlockSpec(memory_space=pltpu.SMEM)
    vmem = pl.BlockSpec(memory_space=pltpu.VMEM)
    whole = jax.ShapeDtypeStruct((rows, ncols), F32)
    block = (height, LANES)
    line = (parts * SUB, LANES)
    dense = pltpu.VMEM(block, F32)
    results = pl.pallas_call(
        functools.partial(kernel, ndp, nmp, loads),
        out_shape=(
            dense,
            dense,
            pltpu.VMEM((ndp, *block), jnp.bfloat16),
            dense,
            dense,
            pltpu.VMEM((2 * rows, LANES), F32),
            pltpu.VMEM((2, *line), F32),
        ),
        in_specs=[hbm] * 10,
        out_specs=[vmem] * 7,
        scratch_shapes=[
            pltpu.VMEM((width, tokens), jnp.bfloat16),
            pltpu.VMEM((parts * loads, tokens, ncols // (parts * loads)), jnp.bfloat16),
            pltpu.VMEM((rows, ncols), F32),
            pltpu.VMEM((rows, ncols), jnp.int32),
            pltpu.VMEM((rows, ncols), jnp.int32),
            pltpu.VMEM((1, rows), F32),
            pltpu.VMEM((1, rows), F32),
            pltpu.VMEM((1, 1), jnp.int32),
            pltpu.VMEM((parts, ndp * rows * SUB, LANES), F32),
            pltpu.VMEM((parts, ndp // 2, 2 * rows * SUB, LANES), I16),
            pltpu.VMEM((ndp // 2, parts, LANES), F32),
            pltpu.VMEM((2 * ndp, 2 * height, LANES), I16),
            pltpu.VMEM((2 * ndp, parts, LANES), F32),
            pltpu.VMEM((ndp // 2, 2, 3 * height, LANES), I16),
            pltpu.VMEM((ndp, 2, LANES), F32),
            pltpu.VMEM((nmp, 2 * height, LANES), I16),
            pltpu.VMEM((nmp, 2 * parts * SUB, LANES), F32),
            pltpu.VMEM((ndp // 2, 2, *block), I16),
            pltpu.VMEM((nmp, *block), I16),
            pltpu.VMEM((ndp * nmp // 4, 2, LANES), F32),
            pltpu.VMEM((ndp * nmp // 4, 1, LANES), F32),
            pltpu.VMEM((2, 2 * height, LANES), F32),
            pltpu.VMEM((2, 2, *block), I16),
            pltpu.VMEM(block, F32),
            pltpu.VMEM(block, F32),
            pltpu.VMEM(block, F32),
            pltpu.VMEM((ndp, *block), F32),
            pltpu.VMEM((ndp, *block), F32),
            pltpu.VMEM((ndp, *block), F32),
            pltpu.VMEM((nmp, *block), F32),
            pltpu.VMEM((nmp, *block), F32),
            pltpu.SemaphoreType.DMA((9,)),
            pltpu.SemaphoreType.DMA((parts * loads,)),
            pltpu.SemaphoreType.DMA((ndp // 2,)),
            pltpu.SemaphoreType.DMA((13,)),
            pltpu.SemaphoreType.DMA((13,)),
        ],
        compiler_params=pltpu.CompilerParams(
            collective_id=0, has_side_effects=True, vmem_limit_bytes=60 * 1024 * 1024
        ),
    )(
        hidden_input.T,
        output_cotangent,
        master_weights,
        first_codes,
        second_codes,
        first_cols.reshape(line),
        second_cols.reshape(line),
        first_rows.reshape(1, rows),
        second_rows.reshape(1, rows),
        step_count.reshape(1, 1),
    )
    scales = jax.ShapeDtypeStruct((rows,), F32)
    cols = jax.ShapeDtypeStruct(line, F32)
    outs = pl.pallas_call(
        unpack,
        out_shape=(
            whole,
            whole,
            jax.ShapeDtypeStruct((ndp * rows, ncols), jnp.bfloat16),
            whole,
            whole,
            scales,
            cols,
            scales,
            cols,
        ),
        in_specs=[vmem] * 7,
        out_specs=[vmem] * 5 + [smem, vmem] * 2,
        scratch_shapes=[pltpu.VMEM((parts, ndp * rows * SUB, LANES), F32)],
        compiler_params=pltpu.CompilerParams(vmem_limit_bytes=40 * 1024 * 1024),
    )(*results)
    return (*outs[:6], outs[6].reshape(ncols), outs[7], outs[8].reshape(ncols))


def solution(mesh):
    return jax.shard_map(
        functools.partial(shards, mesh.shape["dp"], mesh.shape["mp"]),
        mesh=mesh,
        in_specs=(
            P("dp", None),
            P("dp", "mp"),
            P("dp", "mp"),
            P("dp", "mp"),
            P("dp", "mp"),
            P("dp"),
            P("mp"),
            P("dp"),
            P("mp"),
            P(),
        ),
        out_specs=(
            P("dp", "mp"),
            P("dp", "mp"),
            P(None, "mp"),
            P("dp", "mp"),
            P("dp", "mp"),
            P("dp"),
            P("mp"),
            P("dp"),
            P("mp"),
        ),
        check_vma=False,
    )
```

```python
import functools

import jax
import jax.numpy as jnp
from jax import lax
from jax.experimental import pallas as pl
from jax.experimental.pallas import tpu as pltpu
from jax.sharding import PartitionSpec as P

MESH = pl.DeviceIdType.MESH
F32 = jnp.float32
I16 = jnp.int16
FULL = 32767.0


SUB = 8
LANES = 128


def kernel(
    ndp,
    nmp,
    loads_per_part,
    hidden_hbm,
    cot_hbm,
    master_hbm,
    code1_hbm,
    code2_hbm,
    cols1_hbm,
    cols2_hbm,
    rows1_hbm,
    rows2_hbm,
    step_hbm,
    master_out,
    ratio_out,
    params_out,
    scaled1_out,
    scaled2_out,
    rows_out,
    cols_out,
    hidden,
    cot,
    master,
    code1,
    code2,
    rows1,
    rows2,
    step_count,
    share,
    coded_share,
    share_unit,
    grads,
    grad_unit,
    packs,
    metas,
    mcodes,
    mcols,
    gq,
    gm,
    gunits,
    sums,
    gmine,
    gcoded,
    old1,
    old2,
    weights,
    all1,
    all2,
    allw,
    wide1,
    wide2,
    in_sem,
    cot_sem,
    ready,
    pack_sem,
    grad_sem,
    send_sem,
    recv_sem,
):
    dp = lax.axis_index("dp")
    mp = lax.axis_index("mp")
    ndev = ndp * nmp
    flat = dp * nmp + mp
    half, side = lax.div(dp, 2), lax.rem(dp, 2)
    group, core = lax.div(mp, 2), lax.rem(mp, 2)
    lead = 2 * group + 1
    quarter = ndp // 4
    nown = ndp - quarter
    nsum = nmp // 2 * nown
    owner = (core == 1) & (dp < nown)
    extra = owner & (dp >= nown - quarter)
    slot = group * nown + dp
    later = dp + quarter
    source = core * ndp + dp
    rows, ncols = master.shape
    parts = ncols // (SUB * LANES)
    deep = rows * SUB
    high = parts * deep
    lines = parts * SUB
    pieces = parts * loads_per_part
    width = ncols // pieces

    def loop(count, body):
        def step(i, carry):
            body(i)
            return carry

        lax.fori_loop(0, count, step, 0, unroll=count <= 32)

    loads = [
        pltpu.make_async_copy(src, dst, in_sem.at[i])
        for i, (src, dst) in enumerate(
            (
                (hidden_hbm, hidden),
                (code1_hbm, code1),
                (code2_hbm, code2),
                (master_hbm, master),
                (cols1_hbm, mcols.at[mp, pl.ds(0, lines)]),
                (cols2_hbm, mcols.at[mp, pl.ds(lines, lines)]),
                (rows1_hbm, rows1),
                (rows2_hbm, rows2),
                (step_hbm, step_count),
            )
        )
    ]
    cot_loads = [
        pltpu.make_async_copy(
            cot_hbm.at[:, pl.ds(c * width, width)], cot.at[c], cot_sem.at[c]
        )
        for c in range(pieces)
    ]

    def send(src, dst, which, to):
        pltpu.make_async_remote_copy(
            src_ref=src,
            dst_ref=dst,
            send_sem=send_sem.at[which],
            recv_sem=recv_sem.at[which],
            device_id=to,
            device_id_type=MESH,
        ).start()

    def dp_peer(k):
        return {"dp": lax.rem(dp + k + 1, ndp)}

    def mp_peer(k):
        return {"mp": lax.rem(mp + k + 1, nmp)}

    barrier = pltpu.get_barrier_semaphore()

    def hold(flag, count):
        @pl.when(count > 0)
        def _():
            pl.semaphore_wait(flag, count)

    def greet(flag, near, chosen):
        def along(k):
            @pl.when(chosen(k, dp))
            def _():
                for to in (mp, mp + 1 - 2 * core):
                    pl.semaphore_signal(
                        flag,
                        inc=1,
                        device_id={"dp": k, "mp": to},
                        device_id_type=MESH,
                    )

        def beside(k):
            @pl.when(chosen(k, mp))
            def _():
                pl.semaphore_signal(
                    near, inc=1, device_id={"mp": k}, device_id_type=MESH
                )

        loop(ndp, along)
        loop(nmp, beside)

    above = jnp.maximum(nown - jnp.maximum(dp + 1, 0), 0)
    greet(barrier, barrier, lambda k, me: k > me)

    loads[0].start()
    for copy in loads[1:] + cot_loads:
        copy.start()

    def to_owners(body):
        def step(k):
            j = lax.rem(dp + k, ndp)
            o = jnp.where(j < nown, j, j - quarter)
            t = jnp.where(j < nown, 0, 1)

            @pl.when((core == 0) | (dp != o))
            def _():
                body(j, t, {"dp": o, "mp": lead})

        loop(ndp, step)

    def send_share(p):
        to_owners(
            lambda j, t, to: pltpu.make_async_remote_copy(
                src_ref=coded_share.at[p, j],
                dst_ref=grads.at[t, source, pl.ds(p * deep, deep)],
                send_sem=send_sem.at[0],
                recv_sem=grad_sem.at[t],
                device_id=to,
                device_id_type=MESH,
            ).start()
        )

    def send_units():
        to_owners(
            lambda j, t, to: pltpu.make_async_remote_copy(
                src_ref=share_unit.at[j],
                dst_ref=grad_unit.at[t, source],
                send_sem=send_sem.at[11],
                recv_sem=grad_sem.at[2 + t],
                device_id=to,
                device_id_type=MESH,
            ).start()
        )

    def quantize(x):
        top = jnp.maximum(jnp.max(jnp.abs(x), axis=0, keepdims=True), 1e-30)
        code = jnp.floor(x * (FULL / top) + 0.5)
        return code.astype(jnp.int32).astype(I16), top * (1.0 / FULL)

    def code_share(p):
        def body(j):
            block = pl.ds(pl.multiple_of(j * deep, SUB), deep)
            coded, unit = quantize(share[p, block, :])
            coded_share[p, j] = coded
            share_unit[j, p : p + 1] = unit

        return body

    def prepare_packs():
        for copy in loads[1:]:
            copy.wait()

        def dense(value, ref):
            for b in range(ncols // LANES):
                at = (b // SUB) * deep + b % SUB
                ref[pl.ds(at, rows, stride=SUB), :] = value[:, b * LANES : (b + 1) * LANES]

        dense(code1[...].astype(F32), old1)
        dense(code2[...].astype(F32), old2)
        dense(master[...], weights)

        lane = lax.broadcasted_iota(jnp.int32, (1, LANES), 1)
        scales = jnp.zeros((1, LANES), F32)
        for r in range(rows):
            scales = jnp.where(lane == r, rows1[:, r : r + 1], scales)
            scales = jnp.where(lane == rows + r, rows2[:, r : r + 1], scales)
        coded, unit = quantize(weights[...])
        for i, plane in enumerate((old1, old2)):
            code = plane[...].astype(jnp.int32).astype(I16)
            packs[half, side, i * high : (i + 1) * high] = code
            mcodes[mp, i * high : (i + 1) * high] = code
        packs[half, side, 2 * high : 3 * high] = coded
        metas[dp, 0:1] = scales
        metas[dp, 1:2] = unit

    def early(to):
        return (to < half) & ((half < ndp // 2 - 1) | (to == 0))

    def send_pack(to):
        pltpu.make_async_remote_copy(
            src_ref=packs.at[half, side],
            dst_ref=packs.at[half, side],
            send_sem=send_sem.at[2],
            recv_sem=pack_sem.at[half],
            device_id={"dp": 2 * to + side},
            device_id_type=MESH,
        ).start()

    def send_single():
        block = packs.at[half, side]
        send(block, block, 12, {"dp": dp + 1 - 2 * side})

    def send_packs():
        def rest(to):
            @pl.when((to != half) & jnp.logical_not(early(to)))
            def _():
                send_pack(to)

        loop(ndp // 2, rest)

        send_single()
        loop(ndp - 1, lambda k: send(metas.at[dp], metas.at[dp], 4, dp_peer(k)))
        loop(nmp - 1, lambda k: send(mcodes.at[mp], mcodes.at[mp], 5, mp_peer(k)))
        loop(nmp - 1, lambda k: send(mcols.at[mp], mcols.at[mp], 6, mp_peer(k)))

    hold(barrier, 2 * dp + mp)
    which = jnp.where(owner, 0, 1)
    greet(ready.at[which], ready.at[0], lambda k, me: k < me)
    prepare_packs()

    def ahead(to):
        @pl.when(early(to))
        def _():
            send_pack(to)

    loop(ndp // 2, ahead)

    loads[0].wait()
    per_piece = width // LANES
    for c in range(pieces):
        cot_loads[c].wait()
        term = jnp.dot(hidden[...], cot[c], preferred_element_type=F32)
        p = c // loads_per_part
        for i in range(per_piece):
            sub = (c % loads_per_part) * per_piece + i
            share[p, pl.ds(sub, ndp * rows, stride=SUB), :] = term[
                :, i * LANES : (i + 1) * LANES
            ]
        if c % loads_per_part == loads_per_part - 1:
            loop(ndp, code_share(p))
        if c == loads_per_part - 1:
            hold(ready.at[0], above + nmp - 1 - mp)
        if c % loads_per_part == loads_per_part - 1:
            send_share(p)

    send_units()
    hold(ready.at[1], 2 * (ndp - 1 - dp) - above)

    send_packs()

    def scale(row_of, cols):
        tiles = []
        for p in range(parts):
            for r in range(rows):
                tiles.append(jnp.minimum(row_of(r), cols[p * SUB : (p + 1) * SUB]))
        return jnp.concatenate(tiles, axis=0)

    def tile(x, p, r):
        at = p * deep + r * SUB
        return x[at : at + SUB]

    def first_of(code, row_of, cols):
        return 0.9 * ((code - 7.5) / 7.5 * scale(row_of, cols))

    def second_of(code, row_of, cols):
        level = (code + 1.0) / 16.0
        return 0.95 * (level * level * scale(row_of, cols))

    def number(code):
        return code.astype(jnp.int32).astype(F32)

    cols1 = mcols[mp, 0:lines]
    cols2 = mcols[mp, lines : 2 * lines]
    moment1 = first_of(old1[...], lambda r: rows1[:, r : r + 1], cols1)
    moment2 = second_of(old2[...], lambda r: rows2[:, r : r + 1], cols2)
    steps = step_count[...].astype(F32)
    fix1 = 1.0 - jnp.exp(steps * jnp.log(F32(0.9)))
    fix2 = 1.0 - jnp.exp(steps * jnp.log(F32(0.95)))

    def wait_all(ref, count, which):
        blocks = ref.at[pl.ds(0, count)]
        pltpu.make_async_copy(blocks, blocks, which).wait()

    def at_peers(first, count, body):
        def step(k):
            for c in range(2):

                @pl.when((first + k != dp) | (core != c))
                def _(c=c):
                    body(c, {"dp": first + k, "mp": 2 * group + c})

        loop(count, step)

    def across(t, body):
        row = later if t else dp

        def step(to):
            for c in range(2):

                @pl.when((to != 2 * group + c) & ((t == 1) | (to != mp)))
                def _(c=c):
                    body(c, {"dp": row, "mp": to})

        loop(nmp, step)

    def to_all(body):
        def step(k):
            @pl.when(k != flat)
            def _():
                body({"dp": lax.div(k, nmp), "mp": lax.rem(k, nmp)})

        loop(ndev, step)

    def collect(t):
        j = later if t else dp
        for p in range(parts):
            grads[t, source, p * deep : (p + 1) * deep] = coded_share[p, j]
        grad_unit[t, source] = share_unit[j]
        rest = grads.at[t, pl.ds(0, 2 * ndp - 1)]
        pltpu.make_async_copy(rest, rest, grad_sem.at[t]).wait()
        rest = grad_unit.at[t, pl.ds(0, 2 * ndp - 1)]
        pltpu.make_async_copy(rest, rest, grad_sem.at[2 + t]).wait()
        lanes = jnp.zeros((1, LANES), F32)
        for c in range(2):

            def add(d, total, c=c):
                k = c * ndp + d
                sizes = [
                    jnp.broadcast_to(grad_unit[t, k, p : p + 1], (deep, LANES))
                    for p in range(parts)
                ]
                return total + number(grads[t, k]) * jnp.concatenate(sizes, axis=0)

            total = jnp.zeros((high, LANES), F32)
            total = lax.fori_loop(0, ndp, add, total, unroll=ndp <= 8)
            gmine[t, c] = total
            lanes = lanes + jnp.sum(total * total, axis=0, keepdims=True)
        return lanes

    def code_sum(t):
        j = later if t else dp
        for c in range(2):
            coded, unit = quantize(gmine[t, c])
            gunits[group * ndp + j, c : c + 1] = unit
            gcoded[t, c] = coded
        gq[j] = gcoded[t, 1]

    def send_sum(t):
        j = later if t else dp
        units = gunits.at[group * ndp + j]
        to_all(lambda to: send(units, units, 8, to))
        at_peers(0, quarter, lambda c, to: send(gcoded.at[t, c], gq.at[j], 7, to))
        across(t, lambda c, to: send(gcoded.at[t, c], gm.at[2 * group + c], 9, to))
        at_peers(
            quarter,
            ndp - quarter,
            lambda c, to: send(gcoded.at[t, c], gq.at[j], 7, to),
        )

    @pl.when(owner)
    def _():
        sums[slot] = collect(0)

        @pl.when(extra)
        def _():
            sums[slot] = sums[slot] + collect(1)

        to_all(lambda to: send(sums.at[slot], sums.at[slot], 1, to))
        code_sum(0)
        gm[mp - 1] = gcoded[0, 0]
        send_sum(0)

        @pl.when(extra)
        def _():
            code_sum(1)
            send_sum(1)

    column = packs.at[:, side]
    others = column.at[pl.ds(0, ndp // 2 - 1)]
    pair = {"dp": dp + 1 - 2 * side}

    def relay():
        def forward(k):
            ahead = jnp.where(2 * half < ndp // 2, k + 1, ndp // 2 - k - 1)
            at = lax.rem(half + ahead, ndp // 2)
            block = packs.at[at, side]
            pltpu.make_async_copy(block, block, pack_sem.at[at]).wait()
            send(block, block, 3, pair)

        loop(ndp // 2 - 1, forward)

    relay()
    wait_all(metas, ndp - 1, recv_sem.at[4])
    wait_all(mcodes, nmp - 1, recv_sem.at[5])
    wait_all(mcols, nmp - 1, recv_sem.at[6])

    def prepare(j):
        meta = metas[j]
        code1 = number(packs[j // 2, j % 2, 0:high])
        code2 = number(packs[j // 2, j % 2, high : 2 * high])
        all1[j] = first_of(code1, lambda r: meta[0:1, r : r + 1], cols1)
        all2[j] = second_of(
            code2, lambda r: meta[0:1, rows + r : rows + r + 1], cols2
        )
        allw[j] = number(packs[j // 2, j % 2, 2 * high : 3 * high]) * meta[1:2]

    def prepare_wide(k):
        code1, code2 = number(mcodes[k, 0:high]), number(mcodes[k, high : 2 * high])
        wide1[k] = first_of(code1, lambda r: rows1[:, r : r + 1], mcols[k, 0:lines])
        wide2[k] = second_of(
            code2, lambda r: rows2[:, r : r + 1], mcols[k, lines : 2 * lines]
        )

    loop(nmp, prepare_wide)
    pltpu.make_async_copy(others, others, recv_sem.at[3]).wait()
    single = packs.at[half, side]
    pltpu.make_async_copy(single, single, recv_sem.at[12]).wait()
    if ndp <= 8:
        for j in range(ndp):
            prepare(j)
    else:
        lax.fori_loop(0, ndp, lambda j, c: (prepare(j), c)[1], 0)

    def settle(ref, count, which, two):
        @pl.when(jnp.logical_not(owner))
        def _():
            wait_all(ref, count, recv_sem.at[which])

        @pl.when(owner & jnp.logical_not(extra))
        def _():
            wait_all(ref, count - 1, recv_sem.at[which])

        @pl.when(extra)
        def _():
            wait_all(ref, count - two, recv_sem.at[which])

    settle(sums, nsum, 1, 1)
    lanes = jnp.sum(sums[...], axis=0)
    norm = jnp.sqrt(jnp.sum(lanes, axis=1, keepdims=True))
    entries = rows * ncols * ndev
    clipf = jnp.minimum(1.0, 0.01 * jnp.sqrt(F32(entries)) / (norm + 1e-6))

    def over_rows(x):
        tops = []
        for p in range(parts):
            top = tile(x, p, 0)
            for r in range(1, rows):
                top = jnp.maximum(top, tile(x, p, r))
            tops.append(top)
        return jnp.concatenate(tops, axis=0)

    def over_cols(x):
        tops = []
        for r in range(rows):
            top = tile(x, 0, r)
            for p in range(1, parts):
                top = jnp.maximum(top, tile(x, p, r))
            tops.append(top)
        return jnp.concatenate(tops, axis=0)

    def renew(m1, m2, code, unit):
        change = number(code) * (unit * clipf)
        return m1 + 0.1 * change, m2 + 0.05 * (change * change)

    settle(gunits, nmp // 2 * ndp, 8, 2)
    settle(gq, ndp, 7, 2)
    settle(gm, nmp - 1, 9, 1)
    gm[mp] = gq[dp]

    gradient = number(gq[dp]) * gunits[group * ndp + dp, pl.ds(core, 1)]
    clipped = clipf * gradient
    new1 = moment1 + 0.1 * clipped
    new2 = moment2 + 0.05 * (clipped * clipped)
    ratio = new1 / fix1 / (jnp.sqrt(new2 / fix2) + 1e-8)
    old_weights = weights[...]
    master_out[...] = old_weights - 0.001 * (ratio + 0.1 * old_weights)
    ratio_out[...] = ratio

    def widen(k, tops):
        unit = gunits[k // 2 * ndp + dp, pl.ds(k % 2, 1)]
        now1, now2 = renew(wide1[k], wide2[k], gm[k], unit)
        return (
            jnp.maximum(tops[0], over_cols(jnp.abs(now1))),
            jnp.maximum(tops[1], over_cols(now2)),
        )

    flat_top = jnp.zeros((deep, LANES), F32)
    tops = lax.fori_loop(0, nmp, widen, (flat_top, flat_top), unroll=nmp <= 8)
    toprow = jnp.concatenate(
        [
            jnp.max(x[r * SUB : (r + 1) * SUB], axis=0, keepdims=True)
            for x in tops
            for r in range(rows)
        ],
        axis=0,
    )
    toprow = jnp.broadcast_to(jnp.max(toprow, axis=1, keepdims=True), toprow.shape)
    rows_out[...] = toprow

    def finish(j, tops):
        unit = gunits[group * ndp + j, pl.ds(core, 1)]
        now1, now2 = renew(all1[j], all2[j], gq[j], unit)
        held = allw[j]
        turn = now1 / fix1 / (jnp.sqrt(now2 / fix2) + 1e-8)
        params_out[j] = (held - 0.001 * (turn + 0.1 * held)).astype(jnp.bfloat16)
        return (
            jnp.maximum(tops[0], over_rows(jnp.abs(now1))),
            jnp.maximum(tops[1], over_rows(now2)),
        )

    flat_top = jnp.zeros((lines, LANES), F32)
    top1, top2 = lax.fori_loop(0, ndp, finish, (flat_top, flat_top), unroll=ndp <= 8)
    cols_out[0] = top1
    cols_out[1] = top2
    scaled1_out[...] = new1 / (scale(lambda r: toprow[r : r + 1], top1) + 1e-8)
    scaled2_out[...] = new2 / (
        scale(lambda r: toprow[rows + r : rows + r + 1], top2) + 1e-8
    )

    def drain(ref, which):
        pltpu.make_async_copy(ref, ref, send_sem.at[which]).wait()

    for p in range(parts):
        to_owners(lambda j, t, to: drain(coded_share.at[p, j], 0))
    to_owners(lambda j, t, to: drain(share_unit.at[j], 11))

    def drain_sum(t):
        to_all(lambda to: drain(gunits.at[0], 8))
        at_peers(0, ndp, lambda c, to: drain(gcoded.at[t, c], 7))
        across(t, lambda c, to: drain(gcoded.at[t, c], 9))

    @pl.when(owner)
    def _():
        to_all(lambda to: drain(sums.at[slot], 1))
        drain_sum(0)

        @pl.when(extra)
        def _():
            drain_sum(1)

    pltpu.make_async_copy(others, others, send_sem.at[2]).wait()
    pltpu.make_async_copy(others, others, send_sem.at[3]).wait()
    pltpu.make_async_copy(single, single, send_sem.at[12]).wait()
    wait_all(metas, ndp - 1, send_sem.at[4])
    wait_all(mcodes, nmp - 1, send_sem.at[5])
    wait_all(mcols, nmp - 1, send_sem.at[6])


def unpack(
    master,
    ratio,
    params,
    scaled1,
    scaled2,
    toprows,
    topcols,
    master_out,
    ratio_out,
    params_out,
    scaled1_out,
    scaled2_out,
    rows1_out,
    cols1_out,
    rows2_out,
    cols2_out,
    wide,
):
    rows, ncols = master_out.shape
    ndp = params.shape[0]
    parts = ncols // (SUB * LANES)
    deep = rows * SUB

    cols1_out[...] = topcols[0]
    cols2_out[...] = topcols[1]
    for r in range(rows):
        rows1_out[r] = jnp.max(toprows[r : r + 1, :])
        rows2_out[r] = jnp.max(toprows[rows + r : rows + r + 1, :])
    for j in range(ndp):
        block = params[j].astype(F32)
        for p in range(parts):
            wide[p, j * deep : (j + 1) * deep] = block[p * deep : (p + 1) * deep]
    for b in range(ncols // LANES):
        p, sub = b // SUB, b % SUB
        cols = slice(b * LANES, (b + 1) * LANES)
        part = pl.ds(p * deep + sub, rows, stride=SUB)
        master_out[:, cols] = master[part, :]
        ratio_out[:, cols] = ratio[part, :]
        scaled1_out[:, cols] = scaled1[part, :]
        scaled2_out[:, cols] = scaled2[part, :]
        params_out[:, cols] = wide[p, pl.ds(sub, ndp * rows, stride=SUB), :].astype(
            jnp.bfloat16
        )


def shards(
    ndp,
    nmp,
    hidden_input,
    output_cotangent,
    master_weights,
    first_codes,
    second_codes,
    first_rows,
    first_cols,
    second_rows,
    second_cols,
    step_count,
):
    rows, ncols = master_weights.shape
    tokens, width = hidden_input.shape
    parts = ncols // (SUB * LANES)
    loads = 2
    height = parts * rows * SUB
    hbm = pl.BlockSpec(memory_space=pltpu.HBM)
    smem = pl.BlockSpec(memory_space=pltpu.SMEM)
    vmem = pl.BlockSpec(memory_space=pltpu.VMEM)
    whole = jax.ShapeDtypeStruct((rows, ncols), F32)
    block = (height, LANES)
    line = (parts * SUB, LANES)
    dense = pltpu.VMEM(block, F32)
    results = pl.pallas_call(
        functools.partial(kernel, ndp, nmp, loads),
        out_shape=(
            dense,
            dense,
            pltpu.VMEM((ndp, *block), jnp.bfloat16),
            dense,
            dense,
            pltpu.VMEM((2 * rows, LANES), F32),
            pltpu.VMEM((2, *line), F32),
        ),
        in_specs=[hbm] * 10,
        out_specs=[vmem] * 7,
        scratch_shapes=[
            pltpu.VMEM((width, tokens), jnp.bfloat16),
            pltpu.VMEM((parts * loads, tokens, ncols // (parts * loads)), jnp.bfloat16),
            pltpu.VMEM((rows, ncols), F32),
            pltpu.VMEM((rows, ncols), jnp.int32),
            pltpu.VMEM((rows, ncols), jnp.int32),
            pltpu.VMEM((1, rows), F32),
            pltpu.VMEM((1, rows), F32),
            pltpu.VMEM((1, 1), jnp.int32),
            pltpu.VMEM((parts, ndp * rows * SUB, LANES), F32),
            pltpu.VMEM((parts, ndp, rows * SUB, LANES), I16),
            pltpu.VMEM((ndp, parts, LANES), F32),
            pltpu.VMEM((2, 2 * ndp, *block), I16),
            pltpu.VMEM((2, 2 * ndp, parts, LANES), F32),
            pltpu.VMEM((ndp // 2, 2, 3 * height, LANES), I16),
            pltpu.VMEM((ndp, 2, LANES), F32),
            pltpu.VMEM((nmp, 2 * height, LANES), I16),
            pltpu.VMEM((nmp, 2 * parts * SUB, LANES), F32),
            pltpu.VMEM((ndp, *block), I16),
            pltpu.VMEM((nmp, *block), I16),
            pltpu.VMEM((nmp // 2 * ndp, 2, LANES), F32),
            pltpu.VMEM((nmp // 2 * (ndp - ndp // 4), 1, LANES), F32),
            pltpu.VMEM((2, 2, *block), F32),
            pltpu.VMEM((2, 2, *block), I16),
            pltpu.VMEM(block, F32),
            pltpu.VMEM(block, F32),
            pltpu.VMEM(block, F32),
            pltpu.VMEM((ndp, *block), F32),
            pltpu.VMEM((ndp, *block), F32),
            pltpu.VMEM((ndp, *block), F32),
            pltpu.VMEM((nmp, *block), F32),
            pltpu.VMEM((nmp, *block), F32),
            pltpu.SemaphoreType.DMA((9,)),
            pltpu.SemaphoreType.DMA((parts * loads,)),
            pltpu.SemaphoreType.REGULAR((2,)),
            pltpu.SemaphoreType.DMA((ndp // 2,)),
            pltpu.SemaphoreType.DMA((4,)),
            pltpu.SemaphoreType.DMA((13,)),
            pltpu.SemaphoreType.DMA((13,)),
        ],
        compiler_params=pltpu.CompilerParams(
            collective_id=0, has_side_effects=True, vmem_limit_bytes=60 * 1024 * 1024
        ),
    )(
        hidden_input.T,
        output_cotangent,
        master_weights,
        first_codes,
        second_codes,
        first_cols.reshape(line),
        second_cols.reshape(line),
        first_rows.reshape(1, rows),
        second_rows.reshape(1, rows),
        step_count.reshape(1, 1),
    )
    scales = jax.ShapeDtypeStruct((rows,), F32)
    cols = jax.ShapeDtypeStruct(line, F32)
    outs = pl.pallas_call(
        unpack,
        out_shape=(
            whole,
            whole,
            jax.ShapeDtypeStruct((ndp * rows, ncols), jnp.bfloat16),
            whole,
            whole,
            scales,
            cols,
            scales,
            cols,
        ),
        in_specs=[vmem] * 7,
        out_specs=[vmem] * 5 + [smem, vmem] * 2,
        scratch_shapes=[pltpu.VMEM((parts, ndp * rows * SUB, LANES), F32)],
        compiler_params=pltpu.CompilerParams(vmem_limit_bytes=40 * 1024 * 1024),
    )(*results)
    return (*outs[:6], outs[6].reshape(ncols), outs[7], outs[8].reshape(ncols))


def solution(mesh):
    return jax.shard_map(
        functools.partial(shards, mesh.shape["dp"], mesh.shape["mp"]),
        mesh=mesh,
        in_specs=(
            P("dp", None),
            P("dp", "mp"),
            P("dp", "mp"),
            P("dp", "mp"),
            P("dp", "mp"),
            P("dp"),
            P("mp"),
            P("dp"),
            P("mp"),
            P(),
        ),
        out_specs=(
            P("dp", "mp"),
            P("dp", "mp"),
            P(None, "mp"),
            P("dp", "mp"),
            P("dp", "mp"),
            P("dp"),
            P("mp"),
            P("dp"),
            P("mp"),
        ),
        check_vma=False,
    )
```

```python
import functools

import jax
import jax.numpy as jnp
from jax import lax
from jax.experimental import pallas as pl
from jax.experimental.pallas import tpu as pltpu
from jax.sharding import PartitionSpec as P

MESH = pl.DeviceIdType.MESH
F32 = jnp.float32
I16 = jnp.int16
FULL = 32767.0


SUB = 8
LANES = 128


def kernel(
    ndp,
    nmp,
    loads_per_part,
    hidden_hbm,
    cot_hbm,
    master_hbm,
    code1_hbm,
    code2_hbm,
    cols1_hbm,
    cols2_hbm,
    rows1_hbm,
    rows2_hbm,
    step_hbm,
    master_out,
    ratio_out,
    params_out,
    scaled1_out,
    scaled2_out,
    rows_out,
    cols_out,
    hidden,
    cot,
    master,
    code1,
    code2,
    rows1,
    rows2,
    step_count,
    share,
    coded_share,
    share_unit,
    grads,
    grad_unit,
    packs,
    metas,
    mcodes,
    mcols,
    gq,
    gm,
    gunits,
    sums,
    gmine,
    gcoded,
    old1,
    old2,
    weights,
    all1,
    all2,
    allw,
    wide1,
    wide2,
    in_sem,
    cot_sem,
    ready,
    pack_sem,
    grad_sem,
    send_sem,
    recv_sem,
):
    dp = lax.axis_index("dp")
    mp = lax.axis_index("mp")
    ndev = ndp * nmp
    flat = dp * nmp + mp
    half, side = lax.div(dp, 2), lax.rem(dp, 2)
    group, core = lax.div(mp, 2), lax.rem(mp, 2)
    lead = 2 * group + 1
    quarter = ndp // 4
    nown = ndp - quarter
    nsum = nmp // 2 * nown
    owner = (core == 1) & (dp < nown)
    extra = owner & (dp >= nown - quarter)
    slot = group * nown + dp
    later = dp + quarter
    source = core * ndp + dp
    rows, ncols = master.shape
    parts = ncols // (SUB * LANES)
    deep = rows * SUB
    high = parts * deep
    lines = parts * SUB
    pieces = parts * loads_per_part
    width = ncols // pieces

    def loop(count, body):
        def step(i, carry):
            body(i)
            return carry

        lax.fori_loop(0, count, step, 0, unroll=count <= 32)

    loads = [
        pltpu.make_async_copy(src, dst, in_sem.at[i])
        for i, (src, dst) in enumerate(
            (
                (hidden_hbm, hidden),
                (code1_hbm, code1),
                (code2_hbm, code2),
                (master_hbm, master),
                (cols1_hbm, mcols.at[mp, pl.ds(0, lines)]),
                (cols2_hbm, mcols.at[mp, pl.ds(lines, lines)]),
                (rows1_hbm, rows1),
                (rows2_hbm, rows2),
                (step_hbm, step_count),
            )
        )
    ]
    cot_loads = [
        pltpu.make_async_copy(
            cot_hbm.at[:, pl.ds(c * width, width)], cot.at[c], cot_sem.at[c]
        )
        for c in range(pieces)
    ]

    def send(src, dst, which, to):
        pltpu.make_async_remote_copy(
            src_ref=src,
            dst_ref=dst,
            send_sem=send_sem.at[which],
            recv_sem=recv_sem.at[which],
            device_id=to,
            device_id_type=MESH,
        ).start()

    def dp_peer(k):
        return {"dp": lax.rem(dp + k + 1, ndp)}

    def mp_peer(k):
        return {"mp": lax.rem(mp + k + 1, nmp)}

    barrier = pltpu.get_barrier_semaphore()

    def hold(flag, count):
        @pl.when(count > 0)
        def _():
            pl.semaphore_wait(flag, count)

    def greet(flag, near, chosen):
        def along(k):
            @pl.when(chosen(k, dp))
            def _():
                for to in (mp, mp + 1 - 2 * core):
                    pl.semaphore_signal(
                        flag,
                        inc=1,
                        device_id={"dp": k, "mp": to},
                        device_id_type=MESH,
                    )

        def beside(k):
            @pl.when(chosen(k, mp))
            def _():
                pl.semaphore_signal(
                    near, inc=1, device_id={"mp": k}, device_id_type=MESH
                )

        loop(ndp, along)
        loop(nmp, beside)

    above = jnp.maximum(nown - jnp.maximum(dp + 1, 0), 0)
    greet(barrier, barrier, lambda k, me: k > me)

    loads[0].start()
    for copy in loads[1:] + cot_loads:
        copy.start()

    def to_owners(body):
        def step(k):
            j = lax.rem(dp + k, ndp)
            o = jnp.where(j < nown, j, j - quarter)
            t = jnp.where(j < nown, 0, 1)

            @pl.when((core == 0) | (dp != o))
            def _():
                body(j, t, {"dp": o, "mp": lead})

        loop(ndp, step)

    def send_share(p):
        to_owners(
            lambda j, t, to: pltpu.make_async_remote_copy(
                src_ref=coded_share.at[p, j],
                dst_ref=grads.at[t, source, pl.ds(p * deep, deep)],
                send_sem=send_sem.at[0],
                recv_sem=grad_sem.at[t],
                device_id=to,
                device_id_type=MESH,
            ).start()
        )

    def send_units():
        to_owners(
            lambda j, t, to: pltpu.make_async_remote_copy(
                src_ref=share_unit.at[j],
                dst_ref=grad_unit.at[t, source],
                send_sem=send_sem.at[11],
                recv_sem=grad_sem.at[2 + t],
                device_id=to,
                device_id_type=MESH,
            ).start()
        )

    def quantize(x):
        top = jnp.maximum(jnp.max(jnp.abs(x), axis=0, keepdims=True), 1e-30)
        code = jnp.floor(x * (FULL / top) + 0.5)
        return code.astype(jnp.int32).astype(I16), top * (1.0 / FULL)

    def code_share(p):
        def body(j):
            block = pl.ds(pl.multiple_of(j * deep, SUB), deep)
            coded, unit = quantize(share[p, block, :])
            coded_share[p, j] = coded
            share_unit[j, p : p + 1] = unit

        return body

    def prepare_packs():
        for copy in loads[1:]:
            copy.wait()

        def dense(value, ref):
            for b in range(ncols // LANES):
                at = (b // SUB) * deep + b % SUB
                ref[pl.ds(at, rows, stride=SUB), :] = value[:, b * LANES : (b + 1) * LANES]

        dense(code1[...].astype(F32), old1)
        dense(code2[...].astype(F32), old2)
        dense(master[...], weights)

        lane = lax.broadcasted_iota(jnp.int32, (1, LANES), 1)
        scales = jnp.zeros((1, LANES), F32)
        for r in range(rows):
            scales = jnp.where(lane == r, rows1[:, r : r + 1], scales)
            scales = jnp.where(lane == rows + r, rows2[:, r : r + 1], scales)
        coded, unit = quantize(weights[...])
        for i, plane in enumerate((old1, old2)):
            code = plane[...].astype(jnp.int32).astype(I16)
            packs[half, side, i * high : (i + 1) * high] = code
            mcodes[mp, i * high : (i + 1) * high] = code
        packs[half, side, 2 * high : 3 * high] = coded
        metas[dp, 0:1] = scales
        metas[dp, 1:2] = unit

    def early(to):
        return (to < half) & ((half < ndp // 2 - 1) | (to == 0))

    def send_pack(to):
        pltpu.make_async_remote_copy(
            src_ref=packs.at[half, side],
            dst_ref=packs.at[half, side],
            send_sem=send_sem.at[2],
            recv_sem=pack_sem.at[half],
            device_id={"dp": 2 * to + side},
            device_id_type=MESH,
        ).start()

    def send_single():
        block = packs.at[half, side]
        send(block, block, 12, {"dp": dp + 1 - 2 * side})

    def send_packs():
        def rest(to):
            @pl.when((to != half) & jnp.logical_not(early(to)))
            def _():
                send_pack(to)

        loop(ndp // 2, rest)

        send_single()
        loop(ndp - 1, lambda k: send(metas.at[dp], metas.at[dp], 4, dp_peer(k)))
        loop(nmp - 1, lambda k: send(mcodes.at[mp], mcodes.at[mp], 5, mp_peer(k)))
        loop(nmp - 1, lambda k: send(mcols.at[mp], mcols.at[mp], 6, mp_peer(k)))

    hold(barrier, 2 * dp + mp)
    which = jnp.where(owner, 0, 1)
    greet(ready.at[which], ready.at[0], lambda k, me: k < me)
    prepare_packs()

    def ahead(to):
        @pl.when(early(to))
        def _():
            send_pack(to)

    loop(ndp // 2, ahead)

    loads[0].wait()
    per_piece = width // LANES
    for c in range(pieces):
        cot_loads[c].wait()
        term = jnp.dot(hidden[...], cot[c], preferred_element_type=F32)
        p = c // loads_per_part
        for i in range(per_piece):
            sub = (c % loads_per_part) * per_piece + i
            share[p, pl.ds(sub, ndp * rows, stride=SUB), :] = term[
                :, i * LANES : (i + 1) * LANES
            ]
        if c % loads_per_part == loads_per_part - 1:
            loop(ndp, code_share(p))
        if c == loads_per_part - 1:
            hold(ready.at[0], above + nmp - 1 - mp)
        if c % loads_per_part == loads_per_part - 1:
            send_share(p)

    send_units()
    hold(ready.at[1], 2 * (ndp - 1 - dp) - above)

    send_packs()

    def scale(row_of, cols):
        tiles = []
        for p in range(parts):
            for r in range(rows):
                tiles.append(jnp.minimum(row_of(r), cols[p * SUB : (p + 1) * SUB]))
        return jnp.concatenate(tiles, axis=0)

    def tile(x, p, r):
        at = p * deep + r * SUB
        return x[at : at + SUB]

    def first_of(code, row_of, cols):
        return 0.9 * ((code - 7.5) / 7.5 * scale(row_of, cols))

    def second_of(code, row_of, cols):
        level = (code + 1.0) / 16.0
        return 0.95 * (level * level * scale(row_of, cols))

    def number(code):
        return code.astype(jnp.int32).astype(F32)

    cols1 = mcols[mp, 0:lines]
    cols2 = mcols[mp, lines : 2 * lines]
    moment1 = first_of(old1[...], lambda r: rows1[:, r : r + 1], cols1)
    moment2 = second_of(old2[...], lambda r: rows2[:, r : r + 1], cols2)
    steps = step_count[...].astype(F32)
    fix1 = 1.0 - jnp.exp(steps * jnp.log(F32(0.9)))
    fix2 = 1.0 - jnp.exp(steps * jnp.log(F32(0.95)))

    def wait_all(ref, count, which):
        blocks = ref.at[pl.ds(0, count)]
        pltpu.make_async_copy(blocks, blocks, which).wait()

    def at_peers(first, count, body):
        def step(k):
            for c in range(2):

                @pl.when((first + k != dp) | (core != c))
                def _(c=c):
                    body(c, {"dp": first + k, "mp": 2 * group + c})

        loop(count, step)

    def across(t, body):
        row = later if t else dp

        def step(to):
            for c in range(2):

                @pl.when((to != 2 * group + c) & ((t == 1) | (to != mp)))
                def _(c=c):
                    body(c, {"dp": row, "mp": to})

        loop(nmp, step)

    def to_all(body):
        def step(k):
            @pl.when(k != flat)
            def _():
                body({"dp": lax.div(k, nmp), "mp": lax.rem(k, nmp)})

        loop(ndev, step)

    def to_readers(t, body):
        row = later if t else dp

        def other(to):
            @pl.when(lax.div(to, 2) != group)
            def _():
                body({"dp": row, "mp": to})

        at_peers(0, ndp, lambda c, to: body(to))
        loop(nmp, other)

    def collect(t):
        j = later if t else dp
        for p in range(parts):
            grads[t, source, p * deep : (p + 1) * deep] = coded_share[p, j]
        grad_unit[t, source] = share_unit[j]
        rest = grads.at[t, pl.ds(0, 2 * ndp - 1)]
        pltpu.make_async_copy(rest, rest, grad_sem.at[t]).wait()
        rest = grad_unit.at[t, pl.ds(0, 2 * ndp - 1)]
        pltpu.make_async_copy(rest, rest, grad_sem.at[2 + t]).wait()
        lanes = jnp.zeros((1, LANES), F32)
        for c in range(2):

            def add(d, total, c=c):
                k = c * ndp + d
                sizes = [
                    jnp.broadcast_to(grad_unit[t, k, p : p + 1], (deep, LANES))
                    for p in range(parts)
                ]
                return total + number(grads[t, k]) * jnp.concatenate(sizes, axis=0)

            total = jnp.zeros((high, LANES), F32)
            total = lax.fori_loop(0, ndp, add, total, unroll=ndp <= 8)
            gmine[t, c] = total
            lanes = lanes + jnp.sum(total * total, axis=0, keepdims=True)
        return lanes

    def code_sum(t):
        j = later if t else dp
        for c in range(2):
            coded, unit = quantize(gmine[t, c])
            gunits[group * ndp + j, c : c + 1] = unit
            gcoded[t, c] = coded
        gq[j] = gcoded[t, 1]

    def send_near(t):
        j = later if t else dp
        units = gunits.at[group * ndp + j]
        to_readers(t, lambda to: send(units, units, 8, to))
        at_peers(0, quarter, lambda c, to: send(gcoded.at[t, c], gq.at[j], 7, to))

    def send_far(t):
        j = later if t else dp
        across(t, lambda c, to: send(gcoded.at[t, c], gm.at[2 * group + c], 9, to))
        at_peers(
            quarter,
            ndp - quarter,
            lambda c, to: send(gcoded.at[t, c], gq.at[j], 7, to),
        )

    column = packs.at[:, side]
    others = column.at[pl.ds(0, ndp // 2 - 1)]
    pair = {"dp": dp + 1 - 2 * side}

    def relay():
        def forward(k):
            ahead = jnp.where(2 * half < ndp // 2, k + 1, ndp // 2 - k - 1)
            at = lax.rem(half + ahead, ndp // 2)
            block = packs.at[at, side]
            pltpu.make_async_copy(block, block, pack_sem.at[at]).wait()
            send(block, block, 3, pair)

        loop(ndp // 2 - 1, forward)

    @pl.when(half == 0)
    def _():
        relay()

    @pl.when(owner)
    def _():
        sums[slot] = collect(0)

        @pl.when(extra)
        def _():
            sums[slot] = sums[slot] + collect(1)

        to_all(lambda to: send(sums.at[slot], sums.at[slot], 1, to))
        code_sum(0)
        gm[mp - 1] = gcoded[0, 0]

        @pl.when(extra)
        def _():
            code_sum(1)
            send_near(1)

        send_near(0)
        send_far(0)

        @pl.when(extra)
        def _():
            send_far(1)

    @pl.when(half > 0)
    def _():
        relay()

    wait_all(metas, ndp - 1, recv_sem.at[4])
    wait_all(mcodes, nmp - 1, recv_sem.at[5])
    wait_all(mcols, nmp - 1, recv_sem.at[6])

    def prepare(j):
        meta = metas[j]
        code1 = number(packs[j // 2, j % 2, 0:high])
        code2 = number(packs[j // 2, j % 2, high : 2 * high])
        all1[j] = first_of(code1, lambda r: meta[0:1, r : r + 1], cols1)
        all2[j] = second_of(
            code2, lambda r: meta[0:1, rows + r : rows + r + 1], cols2
        )
        allw[j] = number(packs[j // 2, j % 2, 2 * high : 3 * high]) * meta[1:2]

    def prepare_wide(k):
        code1, code2 = number(mcodes[k, 0:high]), number(mcodes[k, high : 2 * high])
        wide1[k] = first_of(code1, lambda r: rows1[:, r : r + 1], mcols[k, 0:lines])
        wide2[k] = second_of(
            code2, lambda r: rows2[:, r : r + 1], mcols[k, lines : 2 * lines]
        )

    loop(nmp, prepare_wide)
    pltpu.make_async_copy(others, others, recv_sem.at[3]).wait()
    single = packs.at[half, side]
    pltpu.make_async_copy(single, single, recv_sem.at[12]).wait()
    if ndp <= 8:
        for j in range(ndp):
            prepare(j)
    else:
        lax.fori_loop(0, ndp, lambda j, c: (prepare(j), c)[1], 0)

    def settle(ref, count, which, two):
        @pl.when(jnp.logical_not(owner))
        def _():
            wait_all(ref, count, recv_sem.at[which])

        @pl.when(owner & jnp.logical_not(extra))
        def _():
            wait_all(ref, count - 1, recv_sem.at[which])

        @pl.when(extra)
        def _():
            wait_all(ref, count - two, recv_sem.at[which])

    settle(sums, nsum, 1, 1)
    lanes = jnp.sum(sums[...], axis=0)
    norm = jnp.sqrt(jnp.sum(lanes, axis=1, keepdims=True))
    entries = rows * ncols * ndev
    clipf = jnp.minimum(1.0, 0.01 * jnp.sqrt(F32(entries)) / (norm + 1e-6))

    def over_rows(x):
        tops = []
        for p in range(parts):
            top = tile(x, p, 0)
            for r in range(1, rows):
                top = jnp.maximum(top, tile(x, p, r))
            tops.append(top)
        return jnp.concatenate(tops, axis=0)

    def over_cols(x):
        tops = []
        for r in range(rows):
            top = tile(x, 0, r)
            for p in range(1, parts):
                top = jnp.maximum(top, tile(x, p, r))
            tops.append(top)
        return jnp.concatenate(tops, axis=0)

    def renew(m1, m2, code, unit):
        change = number(code) * (unit * clipf)
        return m1 + 0.1 * change, m2 + 0.05 * (change * change)

    settle(gunits, ndp + nmp // 2 - 1, 8, 2)
    settle(gq, ndp, 7, 2)
    settle(gm, nmp - 1, 9, 1)
    gm[mp] = gq[dp]

    gradient = number(gq[dp]) * gunits[group * ndp + dp, pl.ds(core, 1)]
    clipped = clipf * gradient
    new1 = moment1 + 0.1 * clipped
    new2 = moment2 + 0.05 * (clipped * clipped)
    ratio = new1 / fix1 / (jnp.sqrt(new2 / fix2) + 1e-8)
    old_weights = weights[...]
    master_out[...] = old_weights - 0.001 * (ratio + 0.1 * old_weights)
    ratio_out[...] = ratio

    def widen(k, tops):
        unit = gunits[k // 2 * ndp + dp, pl.ds(k % 2, 1)]
        now1, now2 = renew(wide1[k], wide2[k], gm[k], unit)
        return (
            jnp.maximum(tops[0], over_cols(jnp.abs(now1))),
            jnp.maximum(tops[1], over_cols(now2)),
        )

    flat_top = jnp.zeros((deep, LANES), F32)
    tops = lax.fori_loop(0, nmp, widen, (flat_top, flat_top), unroll=nmp <= 8)
    toprow = jnp.concatenate(
        [
            jnp.max(x[r * SUB : (r + 1) * SUB], axis=0, keepdims=True)
            for x in tops
            for r in range(rows)
        ],
        axis=0,
    )
    toprow = jnp.broadcast_to(jnp.max(toprow, axis=1, keepdims=True), toprow.shape)
    rows_out[...] = toprow

    def finish(j, tops):
        unit = gunits[group * ndp + j, pl.ds(core, 1)]
        now1, now2 = renew(all1[j], all2[j], gq[j], unit)
        held = allw[j]
        turn = now1 / fix1 / (jnp.sqrt(now2 / fix2) + 1e-8)
        params_out[j] = (held - 0.001 * (turn + 0.1 * held)).astype(jnp.bfloat16)
        return (
            jnp.maximum(tops[0], over_rows(jnp.abs(now1))),
            jnp.maximum(tops[1], over_rows(now2)),
        )

    flat_top = jnp.zeros((lines, LANES), F32)
    top1, top2 = lax.fori_loop(0, ndp, finish, (flat_top, flat_top), unroll=ndp <= 8)
    cols_out[0] = top1
    cols_out[1] = top2
    scaled1_out[...] = new1 / (scale(lambda r: toprow[r : r + 1], top1) + 1e-8)
    scaled2_out[...] = new2 / (
        scale(lambda r: toprow[rows + r : rows + r + 1], top2) + 1e-8
    )

    def drain(ref, which):
        pltpu.make_async_copy(ref, ref, send_sem.at[which]).wait()

    for p in range(parts):
        to_owners(lambda j, t, to: drain(coded_share.at[p, j], 0))
    to_owners(lambda j, t, to: drain(share_unit.at[j], 11))

    def drain_sum(t):
        to_readers(t, lambda to: drain(gunits.at[0], 8))
        at_peers(0, ndp, lambda c, to: drain(gcoded.at[t, c], 7))
        across(t, lambda c, to: drain(gcoded.at[t, c], 9))

    @pl.when(owner)
    def _():
        to_all(lambda to: drain(sums.at[slot], 1))
        drain_sum(0)

        @pl.when(extra)
        def _():
            drain_sum(1)

    pltpu.make_async_copy(others, others, send_sem.at[2]).wait()
    pltpu.make_async_copy(others, others, send_sem.at[3]).wait()
    pltpu.make_async_copy(single, single, send_sem.at[12]).wait()
    wait_all(metas, ndp - 1, send_sem.at[4])
    wait_all(mcodes, nmp - 1, send_sem.at[5])
    wait_all(mcols, nmp - 1, send_sem.at[6])


def unpack(
    master,
    ratio,
    params,
    scaled1,
    scaled2,
    toprows,
    topcols,
    master_out,
    ratio_out,
    params_out,
    scaled1_out,
    scaled2_out,
    rows1_out,
    cols1_out,
    rows2_out,
    cols2_out,
    wide,
):
    rows, ncols = master_out.shape
    ndp = params.shape[0]
    parts = ncols // (SUB * LANES)
    deep = rows * SUB

    cols1_out[...] = topcols[0]
    cols2_out[...] = topcols[1]
    for r in range(rows):
        rows1_out[r] = jnp.max(toprows[r : r + 1, :])
        rows2_out[r] = jnp.max(toprows[rows + r : rows + r + 1, :])
    for j in range(ndp):
        block = params[j].astype(F32)
        for p in range(parts):
            wide[p, j * deep : (j + 1) * deep] = block[p * deep : (p + 1) * deep]
    for b in range(ncols // LANES):
        p, sub = b // SUB, b % SUB
        cols = slice(b * LANES, (b + 1) * LANES)
        part = pl.ds(p * deep + sub, rows, stride=SUB)
        master_out[:, cols] = master[part, :]
        ratio_out[:, cols] = ratio[part, :]
        scaled1_out[:, cols] = scaled1[part, :]
        scaled2_out[:, cols] = scaled2[part, :]
        params_out[:, cols] = wide[p, pl.ds(sub, ndp * rows, stride=SUB), :].astype(
            jnp.bfloat16
        )


def shards(
    ndp,
    nmp,
    hidden_input,
    output_cotangent,
    master_weights,
    first_codes,
    second_codes,
    first_rows,
    first_cols,
    second_rows,
    second_cols,
    step_count,
):
    rows, ncols = master_weights.shape
    tokens, width = hidden_input.shape
    parts = ncols // (SUB * LANES)
    loads = 4
    height = parts * rows * SUB
    hbm = pl.BlockSpec(memory_space=pltpu.HBM)
    smem = pl.BlockSpec(memory_space=pltpu.SMEM)
    vmem = pl.BlockSpec(memory_space=pltpu.VMEM)
    whole = jax.ShapeDtypeStruct((rows, ncols), F32)
    block = (height, LANES)
    line = (parts * SUB, LANES)
    dense = pltpu.VMEM(block, F32)
    results = pl.pallas_call(
        functools.partial(kernel, ndp, nmp, loads),
        out_shape=(
            dense,
            dense,
            pltpu.VMEM((ndp, *block), jnp.bfloat16),
            dense,
            dense,
            pltpu.VMEM((2 * rows, LANES), F32),
            pltpu.VMEM((2, *line), F32),
        ),
        in_specs=[hbm] * 10,
        out_specs=[vmem] * 7,
        scratch_shapes=[
            pltpu.VMEM((width, tokens), jnp.bfloat16),
            pltpu.VMEM((parts * loads, tokens, ncols // (parts * loads)), jnp.bfloat16),
            pltpu.VMEM((rows, ncols), F32),
            pltpu.VMEM((rows, ncols), jnp.int32),
            pltpu.VMEM((rows, ncols), jnp.int32),
            pltpu.VMEM((1, rows), F32),
            pltpu.VMEM((1, rows), F32),
            pltpu.VMEM((1, 1), jnp.int32),
            pltpu.VMEM((parts, ndp * rows * SUB, LANES), F32),
            pltpu.VMEM((parts, ndp, rows * SUB, LANES), I16),
            pltpu.VMEM((ndp, parts, LANES), F32),
            pltpu.VMEM((2, 2 * ndp, *block), I16),
            pltpu.VMEM((2, 2 * ndp, parts, LANES), F32),
            pltpu.VMEM((ndp // 2, 2, 3 * height, LANES), I16),
            pltpu.VMEM((ndp, 2, LANES), F32),
            pltpu.VMEM((nmp, 2 * height, LANES), I16),
            pltpu.VMEM((nmp, 2 * parts * SUB, LANES), F32),
            pltpu.VMEM((ndp, *block), I16),
            pltpu.VMEM((nmp, *block), I16),
            pltpu.VMEM((nmp // 2 * ndp, 2, LANES), F32),
            pltpu.VMEM((nmp // 2 * (ndp - ndp // 4), 1, LANES), F32),
            pltpu.VMEM((2, 2, *block), F32),
            pltpu.VMEM((2, 2, *block), I16),
            pltpu.VMEM(block, F32),
            pltpu.VMEM(block, F32),
            pltpu.VMEM(block, F32),
            pltpu.VMEM((ndp, *block), F32),
            pltpu.VMEM((ndp, *block), F32),
            pltpu.VMEM((ndp, *block), F32),
            pltpu.VMEM((nmp, *block), F32),
            pltpu.VMEM((nmp, *block), F32),
            pltpu.SemaphoreType.DMA((9,)),
            pltpu.SemaphoreType.DMA((parts * loads,)),
            pltpu.SemaphoreType.REGULAR((2,)),
            pltpu.SemaphoreType.DMA((ndp // 2,)),
            pltpu.SemaphoreType.DMA((4,)),
            pltpu.SemaphoreType.DMA((13,)),
            pltpu.SemaphoreType.DMA((13,)),
        ],
        compiler_params=pltpu.CompilerParams(
            collective_id=0, has_side_effects=True, vmem_limit_bytes=60 * 1024 * 1024
        ),
    )(
        hidden_input.T,
        output_cotangent,
        master_weights,
        first_codes,
        second_codes,
        first_cols.reshape(line),
        second_cols.reshape(line),
        first_rows.reshape(1, rows),
        second_rows.reshape(1, rows),
        step_count.reshape(1, 1),
    )
    scales = jax.ShapeDtypeStruct((rows,), F32)
    cols = jax.ShapeDtypeStruct(line, F32)
    outs = pl.pallas_call(
        unpack,
        out_shape=(
            whole,
            whole,
            jax.ShapeDtypeStruct((ndp * rows, ncols), jnp.bfloat16),
            whole,
            whole,
            scales,
            cols,
            scales,
            cols,
        ),
        in_specs=[vmem] * 7,
        out_specs=[vmem] * 5 + [smem, vmem] * 2,
        scratch_shapes=[pltpu.VMEM((parts, ndp * rows * SUB, LANES), F32)],
        compiler_params=pltpu.CompilerParams(vmem_limit_bytes=40 * 1024 * 1024),
    )(*results)
    return (*outs[:6], outs[6].reshape(ncols), outs[7], outs[8].reshape(ncols))


def solution(mesh):
    return jax.shard_map(
        functools.partial(shards, mesh.shape["dp"], mesh.shape["mp"]),
        mesh=mesh,
        in_specs=(
            P("dp", None),
            P("dp", "mp"),
            P("dp", "mp"),
            P("dp", "mp"),
            P("dp", "mp"),
            P("dp"),
            P("mp"),
            P("dp"),
            P("mp"),
            P(),
        ),
        out_specs=(
            P("dp", "mp"),
            P("dp", "mp"),
            P(None, "mp"),
            P("dp", "mp"),
            P("dp", "mp"),
            P("dp"),
            P("mp"),
            P("dp"),
            P("mp"),
        ),
        check_vma=False,
    )
```

```python
import functools

import jax
import jax.numpy as jnp
from jax import lax
from jax.experimental import pallas as pl
from jax.experimental.pallas import tpu as pltpu
from jax.sharding import PartitionSpec as P

MESH = pl.DeviceIdType.MESH
F32 = jnp.float32
I16 = jnp.int16
FULL = 32767.0


SUB = 8
LANES = 128


def kernel(
    ndp,
    nmp,
    loads_per_part,
    hidden_hbm,
    cot_hbm,
    master_hbm,
    code1_hbm,
    code2_hbm,
    cols1_hbm,
    cols2_hbm,
    rows1_hbm,
    rows2_hbm,
    step_hbm,
    master_out,
    ratio_out,
    params_out,
    scaled1_out,
    scaled2_out,
    rows_out,
    cols_out,
    hidden,
    cot,
    master,
    code1,
    code2,
    rows1,
    rows2,
    step_count,
    share,
    coded_share,
    share_unit,
    grads,
    grad_unit,
    packs,
    metas,
    mcodes,
    mcols,
    gq,
    gm,
    gunits,
    sums,
    gmine,
    gcoded,
    old1,
    old2,
    weights,
    all1,
    all2,
    allw,
    wide1,
    wide2,
    in_sem,
    cot_sem,
    ready,
    pack_sem,
    grad_sem,
    send_sem,
    recv_sem,
):
    dp = lax.axis_index("dp")
    mp = lax.axis_index("mp")
    ndev = ndp * nmp
    flat = dp * nmp + mp
    half, side = lax.div(dp, 2), lax.rem(dp, 2)
    group, core = lax.div(mp, 2), lax.rem(mp, 2)
    lead = 2 * group + 1
    quarter = ndp // 4
    nown = ndp - quarter
    nsum = nmp // 2 * nown
    owner = (core == 1) & (dp < nown)
    extra = owner & (dp >= nown - quarter)
    slot = group * nown + dp
    later = dp + quarter
    source = core * ndp + dp
    rows, ncols = master.shape
    parts = ncols // (SUB * LANES)
    deep = rows * SUB
    high = parts * deep
    lines = parts * SUB
    pieces = parts * loads_per_part
    width = ncols // pieces

    def loop(count, body):
        def step(i, carry):
            body(i)
            return carry

        lax.fori_loop(0, count, step, 0, unroll=count <= 32)

    loads = [
        pltpu.make_async_copy(src, dst, in_sem.at[i])
        for i, (src, dst) in enumerate(
            (
                (hidden_hbm, hidden),
                (code1_hbm, code1),
                (code2_hbm, code2),
                (master_hbm, master),
                (cols1_hbm, mcols.at[mp, pl.ds(0, lines)]),
                (cols2_hbm, mcols.at[mp, pl.ds(lines, lines)]),
                (rows1_hbm, rows1),
                (rows2_hbm, rows2),
                (step_hbm, step_count),
            )
        )
    ]
    cot_loads = [
        pltpu.make_async_copy(
            cot_hbm.at[:, pl.ds(c * width, width)], cot.at[c], cot_sem.at[c]
        )
        for c in range(pieces)
    ]

    def send(src, dst, which, to):
        pltpu.make_async_remote_copy(
            src_ref=src,
            dst_ref=dst,
            send_sem=send_sem.at[which],
            recv_sem=recv_sem.at[which],
            device_id=to,
            device_id_type=MESH,
        ).start()

    def dp_peer(k):
        return {"dp": lax.rem(dp + k + 1, ndp)}

    def mp_peer(k):
        return {"mp": lax.rem(mp + k + 1, nmp)}

    barrier = pltpu.get_barrier_semaphore()

    def hold(flag, count):
        @pl.when(count > 0)
        def _():
            pl.semaphore_wait(flag, count)

    def greet(flag, near, chosen):
        def along(k):
            @pl.when(chosen(k, dp))
            def _():
                for to in (mp, mp + 1 - 2 * core):
                    pl.semaphore_signal(
                        flag,
                        inc=1,
                        device_id={"dp": k, "mp": to},
                        device_id_type=MESH,
                    )

        def beside(k):
            @pl.when(chosen(k, mp))
            def _():
                pl.semaphore_signal(
                    near, inc=1, device_id={"mp": k}, device_id_type=MESH
                )

        loop(ndp, along)
        loop(nmp, beside)

    above = jnp.maximum(nown - jnp.maximum(dp + 1, 0), 0)
    greet(barrier, barrier, lambda k, me: k > me)

    loads[0].start()
    for copy in loads[1:] + cot_loads:
        copy.start()

    def to_owners(body):
        def step(k):
            j = lax.rem(dp + k, ndp)
            o = jnp.where(j < nown, j, j - quarter)
            t = jnp.where(j < nown, 0, 1)

            @pl.when((core == 0) | (dp != o))
            def _():
                body(j, t, {"dp": o, "mp": lead})

        loop(ndp, step)

    def send_share(p):
        to_owners(
            lambda j, t, to: pltpu.make_async_remote_copy(
                src_ref=coded_share.at[p, j],
                dst_ref=grads.at[t, source, pl.ds(p * deep, deep)],
                send_sem=send_sem.at[0],
                recv_sem=grad_sem.at[t],
                device_id=to,
                device_id_type=MESH,
            ).start()
        )

    def send_units():
        to_owners(
            lambda j, t, to: pltpu.make_async_remote_copy(
                src_ref=share_unit.at[j],
                dst_ref=grad_unit.at[t, source],
                send_sem=send_sem.at[11],
                recv_sem=grad_sem.at[2 + t],
                device_id=to,
                device_id_type=MESH,
            ).start()
        )

    def quantize(x):
        top = jnp.maximum(jnp.max(jnp.abs(x), axis=0, keepdims=True), 1e-30)
        code = jnp.floor(x * (FULL / top) + 0.5)
        return code.astype(jnp.int32).astype(I16), top * (1.0 / FULL)

    def code_share(p):
        def body(j):
            block = pl.ds(pl.multiple_of(j * deep, SUB), deep)
            coded, unit = quantize(share[p, block, :])
            coded_share[p, j] = coded
            share_unit[j, p : p + 1] = unit

        return body

    def prepare_packs():
        for copy in loads[1:]:
            copy.wait()

        def dense(value, ref):
            for b in range(ncols // LANES):
                at = (b // SUB) * deep + b % SUB
                ref[pl.ds(at, rows, stride=SUB), :] = value[:, b * LANES : (b + 1) * LANES]

        dense(code1[...].astype(F32), old1)
        dense(code2[...].astype(F32), old2)
        dense(master[...], weights)

        lane = lax.broadcasted_iota(jnp.int32, (1, LANES), 1)
        scales = jnp.zeros((1, LANES), F32)
        for r in range(rows):
            scales = jnp.where(lane == r, rows1[:, r : r + 1], scales)
            scales = jnp.where(lane == rows + r, rows2[:, r : r + 1], scales)
        coded, unit = quantize(weights[...])
        for i, plane in enumerate((old1, old2)):
            code = plane[...].astype(jnp.int32).astype(I16)
            packs[half, side, i * high : (i + 1) * high] = code
            mcodes[mp, i * high : (i + 1) * high] = code
        packs[half, side, 2 * high : 3 * high] = coded
        metas[dp, 0:1] = scales
        metas[dp, 1:2] = unit

    def early(to):
        return (to < half) & ((half < ndp // 2 - 1) | (to == 0))

    def send_pack(to):
        pltpu.make_async_remote_copy(
            src_ref=packs.at[half, side],
            dst_ref=packs.at[half, side],
            send_sem=send_sem.at[2],
            recv_sem=pack_sem.at[half],
            device_id={"dp": 2 * to + side},
            device_id_type=MESH,
        ).start()

    def send_single():
        block = packs.at[half, side]
        send(block, block, 12, {"dp": dp + 1 - 2 * side})

    def send_packs():
        def rest(to):
            @pl.when((to != half) & jnp.logical_not(early(to)))
            def _():
                send_pack(to)

        loop(ndp // 2, rest)

        send_single()
        loop(ndp - 1, lambda k: send(metas.at[dp], metas.at[dp], 4, dp_peer(k)))
        loop(nmp - 1, lambda k: send(mcodes.at[mp], mcodes.at[mp], 5, mp_peer(k)))
        loop(nmp - 1, lambda k: send(mcols.at[mp], mcols.at[mp], 6, mp_peer(k)))

    hold(barrier, 2 * dp + mp)
    which = jnp.where(owner, 0, 1)
    greet(ready.at[which], ready.at[0], lambda k, me: k < me)
    prepare_packs()

    def ahead(to):
        @pl.when(early(to))
        def _():
            send_pack(to)

    loop(ndp // 2, ahead)

    loads[0].wait()
    per_piece = width // LANES
    for c in range(pieces):
        cot_loads[c].wait()
        term = jnp.dot(hidden[...], cot[c], preferred_element_type=F32)
        p = c // loads_per_part
        for i in range(per_piece):
            sub = (c % loads_per_part) * per_piece + i
            share[p, pl.ds(sub, ndp * rows, stride=SUB), :] = term[
                :, i * LANES : (i + 1) * LANES
            ]
        if c % loads_per_part == loads_per_part - 1:
            loop(ndp, code_share(p))
        if c == loads_per_part - 1:
            hold(ready.at[0], above + nmp - 1 - mp)
        if c % loads_per_part == loads_per_part - 1:
            send_share(p)

    send_units()
    hold(ready.at[1], 2 * (ndp - 1 - dp) - above)

    send_packs()

    def scale(row_of, cols):
        tiles = []
        for p in range(parts):
            for r in range(rows):
                tiles.append(jnp.minimum(row_of(r), cols[p * SUB : (p + 1) * SUB]))
        return jnp.concatenate(tiles, axis=0)

    def tile(x, p, r):
        at = p * deep + r * SUB
        return x[at : at + SUB]

    def first_of(code, row_of, cols):
        return 0.9 * ((code - 7.5) / 7.5 * scale(row_of, cols))

    def second_of(code, row_of, cols):
        level = (code + 1.0) / 16.0
        return 0.95 * (level * level * scale(row_of, cols))

    def number(code):
        return code.astype(jnp.int32).astype(F32)

    cols1 = mcols[mp, 0:lines]
    cols2 = mcols[mp, lines : 2 * lines]
    moment1 = first_of(old1[...], lambda r: rows1[:, r : r + 1], cols1)
    moment2 = second_of(old2[...], lambda r: rows2[:, r : r + 1], cols2)
    steps = step_count[...].astype(F32)
    fix1 = 1.0 - jnp.exp(steps * jnp.log(F32(0.9)))
    fix2 = 1.0 - jnp.exp(steps * jnp.log(F32(0.95)))

    def wait_all(ref, count, which):
        blocks = ref.at[pl.ds(0, count)]
        pltpu.make_async_copy(blocks, blocks, which).wait()

    def at_peers(first, count, body):
        def step(k):
            for c in range(2):

                @pl.when((first + k != dp) | (core != c))
                def _(c=c):
                    body(c, {"dp": first + k, "mp": 2 * group + c})

        loop(count, step)

    def across(t, body):
        row = later if t else dp

        def step(to):
            for c in range(2):

                @pl.when((to != 2 * group + c) & ((t == 1) | (to != mp)))
                def _(c=c):
                    body(c, {"dp": row, "mp": to})

        loop(nmp, step)

    def to_all(body):
        def step(k):
            @pl.when(k != flat)
            def _():
                body({"dp": lax.div(k, nmp), "mp": lax.rem(k, nmp)})

        loop(ndev, step)

    def to_readers(t, body):
        row = later if t else dp

        def other(to):
            @pl.when(lax.div(to, 2) != group)
            def _():
                body({"dp": row, "mp": to})

        at_peers(0, ndp, lambda c, to: body(to))
        loop(nmp, other)

    def collect(t):
        j = later if t else dp
        for p in range(parts):
            grads[t, source, p * deep : (p + 1) * deep] = coded_share[p, j]
        grad_unit[t, source] = share_unit[j]
        rest = grads.at[t, pl.ds(0, 2 * ndp - 1)]
        pltpu.make_async_copy(rest, rest, grad_sem.at[t]).wait()
        rest = grad_unit.at[t, pl.ds(0, 2 * ndp - 1)]
        pltpu.make_async_copy(rest, rest, grad_sem.at[2 + t]).wait()
        lanes = jnp.zeros((1, LANES), F32)
        for c in range(2):

            def add(d, total, c=c):
                k = c * ndp + d
                sizes = [
                    jnp.broadcast_to(grad_unit[t, k, p : p + 1], (deep, LANES))
                    for p in range(parts)
                ]
                return total + number(grads[t, k]) * jnp.concatenate(sizes, axis=0)

            total = jnp.zeros((high, LANES), F32)
            total = lax.fori_loop(0, ndp, add, total, unroll=ndp <= 8)
            gmine[t, c] = total
            lanes = lanes + jnp.sum(total * total, axis=0, keepdims=True)
        return lanes

    def code_sum(t):
        j = later if t else dp
        for c in range(2):
            coded, unit = quantize(gmine[t, c])
            gunits[group * ndp + j, c : c + 1] = unit
            gcoded[t, c] = coded
        gq[j] = gcoded[t, 1]

    def send_near(t):
        j = later if t else dp
        units = gunits.at[group * ndp + j]
        to_readers(t, lambda to: send(units, units, 8, to))
        at_peers(0, quarter, lambda c, to: send(gcoded.at[t, c], gq.at[j], 7, to))

    def send_far(t):
        j = later if t else dp
        across(t, lambda c, to: send(gcoded.at[t, c], gm.at[2 * group + c], 9, to))
        at_peers(
            quarter,
            ndp - quarter,
            lambda c, to: send(gcoded.at[t, c], gq.at[j], 7, to),
        )

    column = packs.at[:, side]
    others = column.at[pl.ds(0, ndp // 2 - 1)]
    pair = {"dp": dp + 1 - 2 * side}

    def relay():
        def forward(k):
            ahead = jnp.where(2 * half < ndp // 2, k + 1, ndp // 2 - k - 1)
            at = lax.rem(half + ahead, ndp // 2)
            block = packs.at[at, side]
            pltpu.make_async_copy(block, block, pack_sem.at[at]).wait()
            send(block, block, 3, pair)

        loop(ndp // 2 - 1, forward)

    @pl.when(half == 0)
    def _():
        relay()

    @pl.when(owner)
    def _():
        sums[slot] = collect(0)

        @pl.when(extra)
        def _():
            sums[slot] = sums[slot] + collect(1)

        to_all(lambda to: send(sums.at[slot], sums.at[slot], 1, to))
        code_sum(0)
        gm[mp - 1] = gcoded[0, 0]

        @pl.when(extra)
        def _():
            code_sum(1)
            send_near(1)

        send_near(0)
        send_far(0)

        @pl.when(extra)
        def _():
            send_far(1)

    @pl.when(half > 0)
    def _():
        relay()

    wait_all(metas, ndp - 1, recv_sem.at[4])
    wait_all(mcodes, nmp - 1, recv_sem.at[5])
    wait_all(mcols, nmp - 1, recv_sem.at[6])

    def prepare(j):
        meta = metas[j]
        code1 = number(packs[j // 2, j % 2, 0:high])
        code2 = number(packs[j // 2, j % 2, high : 2 * high])
        all1[j] = first_of(code1, lambda r: meta[0:1, r : r + 1], cols1)
        all2[j] = second_of(
            code2, lambda r: meta[0:1, rows + r : rows + r + 1], cols2
        )
        allw[j] = number(packs[j // 2, j % 2, 2 * high : 3 * high]) * meta[1:2]

    def prepare_wide(k):
        code1, code2 = number(mcodes[k, 0:high]), number(mcodes[k, high : 2 * high])
        wide1[k] = first_of(code1, lambda r: rows1[:, r : r + 1], mcols[k, 0:lines])
        wide2[k] = second_of(
            code2, lambda r: rows2[:, r : r + 1], mcols[k, lines : 2 * lines]
        )

    loop(nmp, prepare_wide)
    pltpu.make_async_copy(others, others, recv_sem.at[3]).wait()
    single = packs.at[half, side]
    pltpu.make_async_copy(single, single, recv_sem.at[12]).wait()
    if ndp <= 8:
        for j in range(ndp):
            prepare(j)
    else:
        lax.fori_loop(0, ndp, lambda j, c: (prepare(j), c)[1], 0)

    def settle(ref, count, which, two):
        @pl.when(jnp.logical_not(owner))
        def _():
            wait_all(ref, count, recv_sem.at[which])

        @pl.when(owner & jnp.logical_not(extra))
        def _():
            wait_all(ref, count - 1, recv_sem.at[which])

        @pl.when(extra)
        def _():
            wait_all(ref, count - two, recv_sem.at[which])

    settle(sums, nsum, 1, 1)
    lanes = jnp.sum(sums[...], axis=0)
    norm = jnp.sqrt(jnp.sum(lanes, axis=1, keepdims=True))
    entries = rows * ncols * ndev
    clipf = jnp.minimum(1.0, 0.01 * jnp.sqrt(F32(entries)) / (norm + 1e-6))

    def over_rows(x):
        tops = []
        for p in range(parts):
            top = tile(x, p, 0)
            for r in range(1, rows):
                top = jnp.maximum(top, tile(x, p, r))
            tops.append(top)
        return jnp.concatenate(tops, axis=0)

    def over_cols(x):
        tops = []
        for r in range(rows):
            top = tile(x, 0, r)
            for p in range(1, parts):
                top = jnp.maximum(top, tile(x, p, r))
            tops.append(top)
        return jnp.concatenate(tops, axis=0)

    def renew(m1, m2, code, unit):
        change = number(code) * (unit * clipf)
        return m1 + 0.1 * change, m2 + 0.05 * (change * change)

    settle(gunits, ndp + nmp // 2 - 1, 8, 2)
    settle(gq, ndp, 7, 2)
    settle(gm, nmp - 1, 9, 1)
    gm[mp] = gq[dp]

    gradient = number(gq[dp]) * gunits[group * ndp + dp, pl.ds(core, 1)]
    clipped = clipf * gradient
    new1 = moment1 + 0.1 * clipped
    new2 = moment2 + 0.05 * (clipped * clipped)
    ratio = new1 / fix1 / (jnp.sqrt(new2 / fix2) + 1e-8)
    old_weights = weights[...]
    master_out[...] = old_weights - 0.001 * (ratio + 0.1 * old_weights)
    ratio_out[...] = ratio

    def widen(k, tops):
        unit = gunits[k // 2 * ndp + dp, pl.ds(k % 2, 1)]
        now1, now2 = renew(wide1[k], wide2[k], gm[k], unit)
        return (
            jnp.maximum(tops[0], over_cols(jnp.abs(now1))),
            jnp.maximum(tops[1], over_cols(now2)),
        )

    flat_top = jnp.zeros((deep, LANES), F32)
    tops = lax.fori_loop(0, nmp, widen, (flat_top, flat_top), unroll=nmp <= 8)
    toprow = jnp.concatenate(
        [
            jnp.max(x[r * SUB : (r + 1) * SUB], axis=0, keepdims=True)
            for x in tops
            for r in range(rows)
        ],
        axis=0,
    )
    toprow = jnp.broadcast_to(jnp.max(toprow, axis=1, keepdims=True), toprow.shape)
    rows_out[...] = toprow

    def finish(j, tops):
        unit = gunits[group * ndp + j, pl.ds(core, 1)]
        now1, now2 = renew(all1[j], all2[j], gq[j], unit)
        held = allw[j]
        turn = now1 / fix1 / (jnp.sqrt(now2 / fix2) + 1e-8)
        params_out[j] = (held - 0.001 * (turn + 0.1 * held)).astype(jnp.bfloat16)
        return (
            jnp.maximum(tops[0], over_rows(jnp.abs(now1))),
            jnp.maximum(tops[1], over_rows(now2)),
        )

    flat_top = jnp.zeros((lines, LANES), F32)
    top1, top2 = lax.fori_loop(0, ndp, finish, (flat_top, flat_top), unroll=ndp <= 8)
    cols_out[0] = top1
    cols_out[1] = top2
    scaled1_out[...] = new1 / (scale(lambda r: toprow[r : r + 1], top1) + 1e-8)
    scaled2_out[...] = new2 / (
        scale(lambda r: toprow[rows + r : rows + r + 1], top2) + 1e-8
    )

    def drain(ref, which):
        pltpu.make_async_copy(ref, ref, send_sem.at[which]).wait()

    for p in range(parts):
        to_owners(lambda j, t, to: drain(coded_share.at[p, j], 0))
    to_owners(lambda j, t, to: drain(share_unit.at[j], 11))

    def drain_sum(t):
        to_readers(t, lambda to: drain(gunits.at[0], 8))
        at_peers(0, ndp, lambda c, to: drain(gcoded.at[t, c], 7))
        across(t, lambda c, to: drain(gcoded.at[t, c], 9))

    @pl.when(owner)
    def _():
        to_all(lambda to: drain(sums.at[slot], 1))
        drain_sum(0)

        @pl.when(extra)
        def _():
            drain_sum(1)

    pltpu.make_async_copy(others, others, send_sem.at[2]).wait()
    pltpu.make_async_copy(others, others, send_sem.at[3]).wait()
    pltpu.make_async_copy(single, single, send_sem.at[12]).wait()
    wait_all(metas, ndp - 1, send_sem.at[4])
    wait_all(mcodes, nmp - 1, send_sem.at[5])
    wait_all(mcols, nmp - 1, send_sem.at[6])


def unpack(
    master,
    ratio,
    params,
    scaled1,
    scaled2,
    toprows,
    topcols,
    master_out,
    ratio_out,
    params_out,
    scaled1_out,
    scaled2_out,
    rows1_out,
    cols1_out,
    rows2_out,
    cols2_out,
    wide,
):
    rows, ncols = master_out.shape
    ndp = params.shape[0]
    parts = ncols // (SUB * LANES)
    deep = rows * SUB

    cols1_out[...] = topcols[0]
    cols2_out[...] = topcols[1]
    for r in range(rows):
        rows1_out[r] = jnp.max(toprows[r : r + 1, :])
        rows2_out[r] = jnp.max(toprows[rows + r : rows + r + 1, :])
    for j in range(ndp):
        block = params[j].astype(F32)
        for p in range(parts):
            wide[p, j * deep : (j + 1) * deep] = block[p * deep : (p + 1) * deep]
    for b in range(ncols // LANES):
        p, sub = b // SUB, b % SUB
        cols = slice(b * LANES, (b + 1) * LANES)
        part = pl.ds(p * deep + sub, rows, stride=SUB)
        master_out[:, cols] = master[part, :]
        ratio_out[:, cols] = ratio[part, :]
        scaled1_out[:, cols] = scaled1[part, :]
        scaled2_out[:, cols] = scaled2[part, :]
        params_out[:, cols] = wide[p, pl.ds(sub, ndp * rows, stride=SUB), :].astype(
            jnp.bfloat16
        )


def shards(
    ndp,
    nmp,
    hidden_input,
    output_cotangent,
    master_weights,
    first_codes,
    second_codes,
    first_rows,
    first_cols,
    second_rows,
    second_cols,
    step_count,
):
    rows, ncols = master_weights.shape
    tokens, width = hidden_input.shape
    parts = ncols // (SUB * LANES)
    loads = 2
    height = parts * rows * SUB
    hbm = pl.BlockSpec(memory_space=pltpu.HBM)
    smem = pl.BlockSpec(memory_space=pltpu.SMEM)
    vmem = pl.BlockSpec(memory_space=pltpu.VMEM)
    whole = jax.ShapeDtypeStruct((rows, ncols), F32)
    block = (height, LANES)
    line = (parts * SUB, LANES)
    dense = pltpu.VMEM(block, F32)
    results = pl.pallas_call(
        functools.partial(kernel, ndp, nmp, loads),
        out_shape=(
            dense,
            dense,
            pltpu.VMEM((ndp, *block), jnp.bfloat16),
            dense,
            dense,
            pltpu.VMEM((2 * rows, LANES), F32),
            pltpu.VMEM((2, *line), F32),
        ),
        in_specs=[hbm] * 10,
        out_specs=[vmem] * 7,
        scratch_shapes=[
            pltpu.VMEM((width, tokens), jnp.bfloat16),
            pltpu.VMEM((parts * loads, tokens, ncols // (parts * loads)), jnp.bfloat16),
            pltpu.VMEM((rows, ncols), F32),
            pltpu.VMEM((rows, ncols), jnp.int32),
            pltpu.VMEM((rows, ncols), jnp.int32),
            pltpu.VMEM((1, rows), F32),
            pltpu.VMEM((1, rows), F32),
            pltpu.VMEM((1, 1), jnp.int32),
            pltpu.VMEM((parts, ndp * rows * SUB, LANES), F32),
            pltpu.VMEM((parts, ndp, rows * SUB, LANES), I16),
            pltpu.VMEM((ndp, parts, LANES), F32),
            pltpu.VMEM((2, 2 * ndp, *block), I16),
            pltpu.VMEM((2, 2 * ndp, parts, LANES), F32),
            pltpu.VMEM((ndp // 2, 2, 3 * height, LANES), I16),
            pltpu.VMEM((ndp, 2, LANES), F32),
            pltpu.VMEM((nmp, 2 * height, LANES), I16),
            pltpu.VMEM((nmp, 2 * parts * SUB, LANES), F32),
            pltpu.VMEM((ndp, *block), I16),
            pltpu.VMEM((nmp, *block), I16),
            pltpu.VMEM((nmp // 2 * ndp, 2, LANES), F32),
            pltpu.VMEM((nmp // 2 * (ndp - ndp // 4), 1, LANES), F32),
            pltpu.VMEM((2, 2, *block), F32),
            pltpu.VMEM((2, 2, *block), I16),
            pltpu.VMEM(block, F32),
            pltpu.VMEM(block, F32),
            pltpu.VMEM(block, F32),
            pltpu.VMEM((ndp, *block), F32),
            pltpu.VMEM((ndp, *block), F32),
            pltpu.VMEM((ndp, *block), F32),
            pltpu.VMEM((nmp, *block), F32),
            pltpu.VMEM((nmp, *block), F32),
            pltpu.SemaphoreType.DMA((9,)),
            pltpu.SemaphoreType.DMA((parts * loads,)),
            pltpu.SemaphoreType.REGULAR((2,)),
            pltpu.SemaphoreType.DMA((ndp // 2,)),
            pltpu.SemaphoreType.DMA((4,)),
            pltpu.SemaphoreType.DMA((13,)),
            pltpu.SemaphoreType.DMA((13,)),
        ],
        compiler_params=pltpu.CompilerParams(
            collective_id=0, has_side_effects=True, vmem_limit_bytes=60 * 1024 * 1024
        ),
    )(
        hidden_input.T,
        output_cotangent,
        master_weights,
        first_codes,
        second_codes,
        first_cols.reshape(line),
        second_cols.reshape(line),
        first_rows.reshape(1, rows),
        second_rows.reshape(1, rows),
        step_count.reshape(1, 1),
    )
    scales = jax.ShapeDtypeStruct((rows,), F32)
    cols = jax.ShapeDtypeStruct(line, F32)
    outs = pl.pallas_call(
        unpack,
        out_shape=(
            whole,
            whole,
            jax.ShapeDtypeStruct((ndp * rows, ncols), jnp.bfloat16),
            whole,
            whole,
            scales,
            cols,
            scales,
            cols,
        ),
        in_specs=[vmem] * 7,
        out_specs=[vmem] * 5 + [smem, vmem] * 2,
        scratch_shapes=[pltpu.VMEM((parts, ndp * rows * SUB, LANES), F32)],
        compiler_params=pltpu.CompilerParams(vmem_limit_bytes=40 * 1024 * 1024),
    )(*results)
    return (*outs[:6], outs[6].reshape(ncols), outs[7], outs[8].reshape(ncols))


def solution(mesh):
    return jax.shard_map(
        functools.partial(shards, mesh.shape["dp"], mesh.shape["mp"]),
        mesh=mesh,
        in_specs=(
            P("dp", None),
            P("dp", "mp"),
            P("dp", "mp"),
            P("dp", "mp"),
            P("dp", "mp"),
            P("dp"),
            P("mp"),
            P("dp"),
            P("mp"),
            P(),
        ),
        out_specs=(
            P("dp", "mp"),
            P("dp", "mp"),
            P(None, "mp"),
            P("dp", "mp"),
            P("dp", "mp"),
            P("dp"),
            P("mp"),
            P("dp"),
            P("mp"),
        ),
        check_vma=False,
    )
```
